64 devices in a mesh: dp: 4 (over x, y), tp: 16 (over z, core).
Axes of the slice: x: 2, y: 2, z: 8, core: 2. Of those that a mesh axis runs over, the one named last changes fastest.
The devices are a block of a 4x4x8 slice.
Arguments:
- x_rows: bfloat16 [32768, 4096], P(('dp', 'tp')), parts along dimension 0
- norm_gain: float32 [4096], replicated
- w_q: bfloat16 [4096, 32, 128], P(None, 'tp')
- w_k: bfloat16 [4096, 1024], P(None, 'tp')
- w_v: bfloat16 [4096, 1024], P(None, 'tp')
Outputs:
- output 1: bfloat16 [32768, 32, 128], P('dp', 'tp'), parts along dimension 0
- output 2: bfloat16 [32768, 16, 128], P('dp', 'tp'), parts along dimension 0
- output 3: bfloat16 [32768, 16, 128], P('dp', 'tp'), parts along dimension 0
There are 4 independent parts. The reference program is written for one: setup_inputs(seed, part) draws one part's arguments, and reference() takes and returns one part's arrays. A program takes and returns all parts, laid end to end along the dimension named above; an argument that names none is the same for every part.
All inputs are finite; a program needn't handle non-finite values.
Results may differ from the reference program's by a relative error of at most 0.001.
Values are sent between devices in bfloat16 or wider.
A program may use at most 768 MiB of HBM per device.

```python
import jax
import jax.numpy as jnp
from jax import lax

TOKENS = 8192
D_MODEL = 4096
Q_HEADS = 32
KV_COUNT = 8
HEAD_DIM = 128
GROUP_SIZE = 16
EPSILON = 1e-6


def setup_inputs(seed: int = 0, part: int = 0) -> dict:
    key = jax.random.key(seed)
    shared_key, rows_key = jax.random.split(key)
    part_key = jax.random.fold_in(rows_key, part)
    x_rows = jax.random.normal(part_key, (TOKENS, D_MODEL), jnp.float32).astype(jnp.bfloat16)
    gain_key, q_key, k_key, v_key = jax.random.split(shared_key, 4)
    norm_gain = jax.random.uniform(gain_key, (D_MODEL,), jnp.float32, 0.4, 1.6)
    weight_scale = D_MODEL ** -0.5
    w_q = (jax.random.normal(q_key, (D_MODEL, Q_HEADS, HEAD_DIM), jnp.float32) * weight_scale).astype(jnp.bfloat16)
    w_k = (jax.random.normal(k_key, (D_MODEL, KV_COUNT * HEAD_DIM), jnp.float32) * weight_scale).astype(jnp.bfloat16)
    w_v = (jax.random.normal(v_key, (D_MODEL, KV_COUNT * HEAD_DIM), jnp.float32) * weight_scale).astype(jnp.bfloat16)
    return {"x_rows": x_rows, "norm_gain": norm_gain, "w_q": w_q, "w_k": w_k, "w_v": w_v}


def reference(x_rows, norm_gain, w_q, w_k, w_v):
    x_wide = x_rows.astype(jnp.float32)
    mean_sq = jnp.mean(x_wide * x_wide, axis=-1, keepdims=True)
    normed = (x_wide * lax.rsqrt(mean_sq + EPSILON) * norm_gain).astype(jnp.bfloat16)
    q_flat = jnp.dot(normed, w_q.reshape(D_MODEL, Q_HEADS * HEAD_DIM), preferred_element_type=jnp.float32)
    q_out = q_flat.astype(jnp.bfloat16).reshape(TOKENS, Q_HEADS, HEAD_DIM)
    head_share = GROUP_SIZE // KV_COUNT
    k_flat = jnp.dot(normed, w_k, preferred_element_type=jnp.float32).astype(jnp.bfloat16)
    v_flat = jnp.dot(normed, w_v, preferred_element_type=jnp.float32).astype(jnp.bfloat16)
    k_out = jnp.repeat(k_flat.reshape(TOKENS, KV_COUNT, HEAD_DIM), head_share, axis=1)
    v_out = jnp.repeat(v_flat.reshape(TOKENS, KV_COUNT, HEAD_DIM), head_share, axis=1)
    return (q_out, k_out, v_out)
```

```python
import functools
import math

import jax
import jax.numpy as jnp
from jax import lax
from jax.experimental import pallas as pl
from jax.experimental.pallas import tpu as pltpu
from jax.sharding import PartitionSpec as P

EPSILON = 1e-6
MESH = pl.DeviceIdType.MESH
CORES = 2
QUARTERS = 4
HALVES = 2
CHUNKS = QUARTERS * HALVES
TILE = 256
NORM_ROWS = 16
ORDER = (7, 2, 6, 4, 3, 5, 1)


def kernel(ring, side, x_hbm, gain_hbm, wq_hbm, wk_hbm, wv_hbm, q_out, kv_out,
           rows, gain, wq, wkv, wflat, oq, okv,
           local_sem, x_send, x_recv, pair_send, pair_recv, z_send, z_recv, xy_send, xy_recv,
           oq_send, okv_send, oq_recv, okv_recv, fw_send, fw_recv, keep_sem):
    dp, tp = lax.axis_index("dp"), lax.axis_index("tp")
    z, c = tp // CORES, tp % CORES
    grid_x, grid_y = dp // side, dp % side
    odd_x, odd_y = grid_x % 2, grid_y % 2
    quarter = 2 * odd_x + odd_y
    quarter_x, quarter_y, quarter_d = 2 * (1 - odd_x) + odd_y, 2 * odd_x + 1 - odd_y, 3 - quarter
    x_peer = (dp + side * (1 - 2 * odd_x), tp)
    y_peer = (dp + 1 - 2 * odd_y, tp)
    partner = (dp, tp + 1 - 2 * c)

    own, depth = x_hbm.shape
    chip_rows = CORES * own
    step = depth // CHUNKS
    piece = wk_hbm.shape[0]
    tiles = chip_rows // TILE

    def at_ring(distance):
        return (dp, CORES * ((z + ring - distance) % ring) + c)

    def remote(src, dst, send, recv, device):
        return pltpu.make_async_remote_copy(src_ref=src, dst_ref=dst, send_sem=send, recv_sem=recv, device_id=device, device_id_type=MESH)

    def part(block, chunk):
        first = pl.multiple_of(chunk * step, step)
        return wq.at[block, pl.ds(first, step)], wkv.at[block, chunk]

    own_first = pl.multiple_of(c * own, own)
    lane = own // 4
    x_loads = [pltpu.make_async_copy(x_hbm.at[pl.ds(i * lane, lane)], rows.at[pl.ds(own_first + i * lane, lane)], local_sem.at[i]) for i in range(4)]
    w_loads = []
    for i in range(QUARTERS):
        first = pl.multiple_of(((quarter + i) % QUARTERS) * (depth // QUARTERS), depth // QUARTERS)
        w_loads.append(pltpu.make_async_copy(wq_hbm.at[pl.ds(first, depth // QUARTERS)], wq.at[z, pl.ds(first, depth // QUARTERS)], local_sem.at[4 + i]))
    gain_load = pltpu.make_async_copy(gain_hbm, gain, local_sem.at[8])
    own_half = pl.ds(pl.multiple_of(c * piece, piece), piece)

    def columns(i):
        chunk = (HALVES * quarter + i) % CHUNKS
        return chunk, pl.ds(pl.multiple_of(chunk * step, step), step)

    def pair_load(source, i):
        chunk, span = columns(i)
        return pltpu.make_async_copy(source.at[:, span], wkv.at[z, chunk, own_half], local_sem.at[9 + i])

    def pair_copy(source, i):
        chunk, span = columns(i)
        return remote(source.at[:, span], wkv.at[z, chunk, own_half], pair_send.at[i], pair_recv.at[i], partner)

    def pair_arrival(i):
        chunk, span = columns(i)
        other_half = pl.ds(pl.multiple_of((1 - c) * piece, piece), piece)
        return remote(wk_hbm.at[:, span], wkv.at[z, chunk, other_half], pair_send.at[i], pair_recv.at[i], partner)

    w_loads[0].start()
    for load in x_loads:
        load.start()
    gain_load.start()

    @pl.when(c == 0)
    def _():
        for i in range(CHUNKS):
            pair_load(wk_hbm, i).start()

    @pl.when(c == 1)
    def _():
        for i in range(CHUNKS):
            pair_load(wv_hbm, i).start()

    for load in w_loads[1:]:
        load.start()

    barrier = pltpu.get_barrier_semaphore()
    peers = [x_peer, y_peer, partner] + [at_ring(r) for r in range(1, ring)]
    for peer in peers:
        pl.semaphore_signal(barrier, inc=1, device_id=peer, device_id_type=MESH)
    pl.semaphore_wait(barrier, len(peers))

    @pl.when(c == 0)
    def _():
        for i in range(CHUNKS):
            pair_copy(wv_hbm, i).start()

    @pl.when(c == 1)
    def _():
        for i in range(CHUNKS):
            pair_copy(wk_hbm, i).start()

    half_ring = ring // 2
    started = []

    def ring_send(direction, hop, half, kind):
        back = hop if direction == 0 else ring - hop
        block = (z + ring - back) % ring
        reference = part(block, HALVES * quarter + half)[kind]
        index = ((back * HALVES + half) * 2 + kind) if hop else ((direction * ring * HALVES + half) * 2 + kind)
        landed = (hop + 1) if direction == 0 else ring - hop - 1
        copy = remote(reference, reference, z_send.at[index], z_recv.at[(landed * HALVES + half) * 2 + kind], at_ring(ring - 1 if direction == 0 else 1))
        copy.start()
        started.append(copy)

    def reach(direction, half):
        return half_ring if direction == half else half_ring - 1

    def ring_arrival(direction, hop, half, kind):
        back = hop if direction == 0 else ring - hop
        block = (z + ring - back) % ring
        reference = part(block, HALVES * quarter + half)[kind]
        remote(reference, reference, z_send.at[0], z_recv.at[(back * HALVES + half) * 2 + kind], at_ring(1)).wait_recv()

    def ring_service(hop, half):
        for kind in range(2):
            for direction in range(2):
                if hop <= reach(direction, half):
                    ring_arrival(direction, hop, half, kind)
                    if hop < reach(direction, half):
                        ring_send(direction, hop, half, kind)

    def square_copy(r, lane_index, chunk, kind, device):
        block = (z + ring - r) % ring
        reference = part(block, chunk)[kind]
        index = (r * 6 + lane_index) * 2 + kind
        return remote(reference, reference, xy_send.at[index], xy_recv.at[index], device)

    def square_send(r, half):
        for kind in range(2):
            for base, device in ((0, x_peer), (2, y_peer)):
                copy = square_copy(r, base + half, HALVES * quarter + half, kind, device)
                copy.start()
                started.append(copy)

    def square_forward(r, half):
        base, chunk, device = ((0, HALVES * quarter_x, y_peer), (2, HALVES * quarter_y, x_peer))[half]
        for kind in range(2):
            square_copy(r, base + half, chunk + half, kind, device).wait_recv()
            copy = square_copy(r, 4 + half, chunk + half, kind, device)
            copy.start()
            started.append(copy)

    def square_rest(r):
        for kind in range(2):
            square_copy(r, 1, HALVES * quarter_x + 1, kind, x_peer).wait_recv()
            square_copy(r, 2, HALVES * quarter_y, kind, y_peer).wait_recv()
            square_copy(r, 4, HALVES * quarter_d, kind, y_peer).wait_recv()
            square_copy(r, 5, HALVES * quarter_d + 1, kind, x_peer).wait_recv()

    def flatten(block):
        @pl.loop(0, CHUNKS)
        def _(i):
            span = pl.ds(pl.multiple_of(i * step, step), step)
            wflat[span, :] = wq[block, span].reshape(step, wflat.shape[1])

    def product(block, slot, first):
        span = pl.ds(first, TILE)
        q = jnp.dot(rows[span, :], wflat[...], preferred_element_type=jnp.float32)
        oq[slot, span] = q.reshape((TILE,) + oq.shape[2:]).astype(oq.dtype)
        kv = jnp.zeros((TILE, okv.shape[2]), jnp.float32)
        for i in range(CHUNKS):
            kv += lax.dot_general(rows[span, pl.ds(i * step, step)], wkv[block, i], (((1,), (1,)), ((), ())), preferred_element_type=jnp.float32)
        okv[slot, span] = kv.astype(okv.dtype)

    def out_rows(block, first, count):
        return pl.ds(pl.multiple_of(block * chip_rows + first, TILE), count)

    def out_copies(r, first, count):
        span, target = pl.ds(first, count), out_rows(z, first, count)
        return (
            remote(oq.at[r, span], q_out.at[target], oq_send.at[r], oq_recv.at[r], at_ring(r)),
            remote(okv.at[r, span], kv_out.at[c, target], okv_send.at[r], okv_recv.at[r], at_ring(r)),
        )

    def multiply(r):
        block = (z + ring - r) % ring
        flatten(block)

        @pl.loop(0, tiles)
        def _(t):
            first = pl.multiple_of(t * TILE, TILE)
            product(block, r, first)
            for copy in out_copies(r, first, TILE):
                copy.start()

    def keep_copies():
        target = out_rows(z, 0, chip_rows)
        return (
            pltpu.make_async_copy(oq.at[0], q_out.at[target], keep_sem.at[0]),
            pltpu.make_async_copy(okv.at[0], kv_out.at[c, target], keep_sem.at[1]),
        )

    def hand_over(r, source):
        target = out_rows((z + r) % ring, 0, chip_rows)
        return remote(source, kv_out.at[c, target], fw_send.at[r], fw_recv.at[r], partner)

    def hand_arrival(r):
        target = out_rows((z + r) % ring, 0, chip_rows)
        return remote(okv.at[0], kv_out.at[1 - c, target], fw_send.at[r], fw_recv.at[r], partner)

    def relay(r):
        target = out_rows((z + r) % ring, 0, chip_rows)
        remote(okv.at[r], kv_out.at[c, target], okv_send.at[r], okv_recv.at[r], at_ring(r)).wait_recv()
        hand_over(r, kv_out.at[c, target]).start()

    w_loads[0].wait()
    for half in range(HALVES):
        for direction in range(2):
            ring_send(direction, 0, half, 0)
    for i in range(CHUNKS):
        pair_load(wk_hbm, i).wait()
    for half in range(HALVES):
        pair_arrival(half).wait_recv()
        for direction in range(2):
            ring_send(direction, 0, half, 1)

    gain_load.wait()
    for i in range(4):
        x_loads[i].wait()

        @pl.loop(0, lane // NORM_ROWS)
        def _(n):
            span = pl.ds(pl.multiple_of(own_first + i * lane + n * NORM_ROWS, NORM_ROWS), NORM_ROWS)
            wide = rows[span, :].astype(jnp.float32)
            mean_sq = jnp.mean(wide * wide, axis=-1, keepdims=True)
            rows[span, :] = (wide * lax.rsqrt(mean_sq + EPSILON) * gain[...]).astype(rows.dtype)

        span = pl.ds(own_first + i * lane, lane)
        remote(rows.at[span], rows.at[span], x_send.at[i], x_recv.at[i], partner).start()

    ring_service(1, 0)
    square_send(ORDER[0], 0)

    for i in range(4):
        span = pl.ds(pl.multiple_of((1 - c) * own + i * lane, lane), lane)
        remote(rows.at[span], rows.at[span], x_send.at[i], x_recv.at[i], partner).wait_recv()
    for load in w_loads[1:]:
        load.wait()
    for i in range(HALVES, CHUNKS):
        pair_arrival(i).wait_recv()
    flatten(z)

    def own_products(first_tile, count):
        @pl.loop(first_tile, first_tile + count)
        def _(t):
            product(z, 0, pl.multiple_of(t * TILE, TILE))

    own_products(0, tiles // 2)
    ring_service(1, 1)
    square_send(ORDER[0], 1)
    own_products(tiles // 2, tiles - tiles // 2)
    for copy in keep_copies():
        copy.start()
    hand_over(0, okv.at[0]).start()
    square_forward(ORDER[0], 0)
    ring_service(2, 0)
    square_send(ORDER[1], 0)

    services = {(0, 0): ((2, 1),), (0, 1): ((3, 0),), (1, 0): ((3, 1),), (1, 1): ((4, 0),), (2, 0): ((4, 1),)}
    blocks = len(ORDER)
    for j in range(blocks):
        square_forward(ORDER[j], 1)
        for hop, half in services.get((j, 0), ()):
            ring_service(hop, half)
        if j + 1 < blocks:
            square_send(ORDER[j + 1], 1)
            square_forward(ORDER[j + 1], 0)
        for hop, half in services.get((j, 1), ()):
            ring_service(hop, half)
        if j + 2 < blocks:
            square_send(ORDER[j + 2], 0)
        square_rest(ORDER[j])
        multiply(ORDER[j])
        if j >= 3:
            relay(ORDER[j - 3])

    for r in ORDER[blocks - 3:]:
        relay(r)
    for r in ORDER:
        target = out_rows((z + r) % ring, 0, chip_rows)
        remote(oq.at[r], q_out.at[target], oq_send.at[r], oq_recv.at[r], at_ring(r)).wait_recv()
    for r in range(ring):
        hand_arrival(r).wait_recv()

    for copy in keep_copies():
        copy.wait()
    for copy in started:
        copy.wait_send()
    for r in ORDER:
        for copy in out_copies(r, 0, chip_rows):
            copy.wait_send()
    for r in range(ring):
        hand_over(r, okv.at[0]).wait_send()
    for i in range(4):
        span = pl.ds(own_first + i * lane, lane)
        remote(rows.at[span], rows.at[span], x_send.at[i], x_recv.at[i], partner).wait_send()
    for i in range(CHUNKS):
        pair_copy(wk_hbm, i).wait_send()


def solution(mesh):
    ring = mesh.shape["tp"] // CORES
    side = math.isqrt(mesh.shape["dp"])
    assert side * side == mesh.shape["dp"] and side % 2 == 0

    def local_step(x_rows, norm_gain, w_q, w_k, w_v):
        own, depth = x_rows.shape
        heads, width = w_q.shape[1:]
        piece = w_k.shape[1]
        assert piece * CORES == width
        tokens, chip_rows, step = own * CORES * ring, own * CORES, depth // CHUNKS
        dma = pltpu.SemaphoreType.DMA
        bf16 = x_rows.dtype
        q_out, kv_out = pl.pallas_call(
            functools.partial(kernel, ring, side),
            out_shape=(
                jax.ShapeDtypeStruct((tokens, heads, width), bf16),
                jax.ShapeDtypeStruct((CORES, tokens, width), bf16),
            ),
            in_specs=[pl.BlockSpec(memory_space=pl.ANY)] * 5,
            out_specs=(pl.BlockSpec(memory_space=pl.ANY),) * 2,
            scratch_shapes=[
                pltpu.VMEM((chip_rows, depth), bf16),
                pltpu.VMEM((1, depth), jnp.float32),
                pltpu.VMEM((ring, depth, heads, width), bf16),
                pltpu.VMEM((ring, CHUNKS, width, step), bf16),
                pltpu.VMEM((depth, heads * width), bf16),
                pltpu.VMEM((ring, chip_rows, heads, width), bf16),
                pltpu.VMEM((ring, chip_rows, width), bf16),
                dma((9 + CHUNKS,)),
                dma((4,)), dma((4,)),
                dma((CHUNKS,)), dma((CHUNKS,)),
                dma((2 * ring * HALVES * 2,)), dma((ring * HALVES * 2,)),
                dma((ring * 6 * 2,)), dma((ring * 6 * 2,)),
                dma((ring,)), dma((ring,)), dma((ring,)), dma((ring,)),
                dma((ring,)), dma((ring,)),
                dma((2,)),
            ],
            compiler_params=pltpu.CompilerParams(collective_id=0, has_side_effects=True, vmem_limit_bytes=56 * 1024 * 1024),
        )(x_rows, norm_gain.reshape(1, depth), w_q, w_k.T, w_v.T)
        return q_out, kv_out[0][:, None, :], kv_out[1][:, None, :]

    return jax.shard_map(local_step, mesh=mesh, in_specs=(P(("dp", "tp"), None), P(None), P(None, "tp", None), P(None, "tp"), P(None, "tp")), out_specs=(P("dp", "tp", None), P("dp", "tp", None), P("dp", "tp", None)), check_vma=False)
```

```python
import functools
import math

import jax
import jax.numpy as jnp
from jax import lax
from jax.experimental import pallas as pl
from jax.experimental.pallas import tpu as pltpu
from jax.sharding import PartitionSpec as P

EPSILON = 1e-6
MESH = pl.DeviceIdType.MESH
CORES = 2
QUARTERS = 4
HALVES = 2
CHUNKS = QUARTERS * HALVES
TILE = 256
NORM_ROWS = 16

ARRIVE, SPREAD, FORWARD, MULTIPLY, HAND_OVER, NORM, OWN = range(7)
SCHEDULE = (
    (NORM, 0, 0, 0), (NORM, 0, 0, 0), (NORM, 0, 0, 0), (ARRIVE, 1, 1, 0), (SPREAD, 7, 1, 0),
    (NORM, 0, 0, 0), (OWN, 0, 1, 0), (ARRIVE, 1, 1, 1), (SPREAD, 7, 1, 1), (SPREAD, 1, 1, 0),
    (SPREAD, 1, 1, 1), (OWN, 0, 0, 0), (ARRIVE, 1, 0, 0), (FORWARD, 7, 1, 0), (FORWARD, 7, 1, 1),
    (FORWARD, 1, 1, 0), (ARRIVE, 1, 0, 1), (FORWARD, 1, 1, 1), (ARRIVE, 2, 1, 0), (SPREAD, 2, 1, 0),
    (MULTIPLY, 7, 1, 0), (ARRIVE, 2, 1, 1), (SPREAD, 2, 1, 1), (MULTIPLY, 1, 1, 0), (ARRIVE, 2, 0, 0),
    (FORWARD, 2, 1, 0), (SPREAD, 2, 0, 0), (FORWARD, 2, 1, 1), (ARRIVE, 2, 0, 1), (SPREAD, 2, 0, 1),
    (SPREAD, 6, 1, 0), (SPREAD, 6, 1, 1), (ARRIVE, 3, 1, 0), (MULTIPLY, 2, 1, 0), (FORWARD, 2, 0, 0),
    (HAND_OVER, 7, 1, 0), (FORWARD, 2, 0, 1), (ARRIVE, 3, 1, 1), (HAND_OVER, 1, 1, 0), (FORWARD, 6, 1, 0),
    (FORWARD, 6, 1, 1), (ARRIVE, 3, 0, 0), (SPREAD, 5, 0, 0), (MULTIPLY, 2, 0, 0), (ARRIVE, 3, 0, 1),
    (ARRIVE, 4, 1, 0), (SPREAD, 5, 0, 1), (SPREAD, 4, 1, 0), (MULTIPLY, 6, 1, 0), (FORWARD, 5, 0, 0),
    (ARRIVE, 4, 0, 0), (HAND_OVER, 2, 1, 0), (FORWARD, 5, 0, 1), (ARRIVE, 4, 1, 1), (SPREAD, 4, 1, 1),
    (SPREAD, 3, 0, 0), (SPREAD, 3, 0, 1), (FORWARD, 4, 1, 0), (HAND_OVER, 6, 1, 0), (SPREAD, 5, 1, 0),
    (MULTIPLY, 5, 0, 0), (FORWARD, 4, 1, 1), (SPREAD, 5, 1, 1), (SPREAD, 4, 0, 0), (FORWARD, 3, 0, 0),
    (FORWARD, 3, 0, 1), (MULTIPLY, 4, 1, 0), (ARRIVE, 4, 0, 1), (FORWARD, 5, 1, 0), (FORWARD, 5, 1, 1),
    (SPREAD, 4, 0, 1), (SPREAD, 6, 0, 0), (FORWARD, 4, 0, 0), (SPREAD, 6, 0, 1), (MULTIPLY, 3, 0, 0),
    (SPREAD, 3, 1, 0), (MULTIPLY, 5, 1, 0), (FORWARD, 4, 0, 1), (SPREAD, 3, 1, 1), (FORWARD, 6, 0, 0),
    (HAND_OVER, 4, 1, 0), (SPREAD, 7, 0, 0), (SPREAD, 7, 0, 1), (FORWARD, 6, 0, 1), (MULTIPLY, 4, 0, 0),
    (FORWARD, 3, 1, 0), (FORWARD, 3, 1, 1), (HAND_OVER, 5, 1, 0), (SPREAD, 1, 0, 0), (SPREAD, 1, 0, 1),
    (FORWARD, 7, 0, 0), (MULTIPLY, 6, 0, 0), (FORWARD, 7, 0, 1), (MULTIPLY, 3, 1, 0), (FORWARD, 1, 0, 0),
    (FORWARD, 1, 0, 1), (MULTIPLY, 7, 0, 0), (MULTIPLY, 1, 0, 0), (HAND_OVER, 3, 1, 0),
)


def kernel(ring, side, x_hbm, gain_hbm, wq_hbm, wk_hbm, wv_hbm, q_out, kv_out,
           rows, gain, wq, wkv, wflat, oq, okv,
           local_sem, x_send, x_recv, pair_send, pair_recv, z_send, z_recv, xy_send, xy_recv,
           oq_send, okv_send, oq_recv, okv_recv, fw_send, fw_recv, keep_sem):
    dp, tp = lax.axis_index("dp"), lax.axis_index("tp")
    z, c = tp // CORES, tp % CORES
    grid_x, grid_y = dp // side, dp % side
    odd_x, odd_y = grid_x % 2, grid_y % 2
    quarter = 2 * odd_x + odd_y
    quarter_x, quarter_y, quarter_d = 2 * (1 - odd_x) + odd_y, 2 * odd_x + 1 - odd_y, 3 - quarter
    x_peer = (dp + side * (1 - 2 * odd_x), tp)
    y_peer = (dp + 1 - 2 * odd_y, tp)
    partner = (dp, tp + 1 - 2 * c)

    own, depth = x_hbm.shape
    chip_rows = CORES * own
    step = depth // CHUNKS
    piece = wk_hbm.shape[0]
    tiles = chip_rows // TILE

    def at_ring(distance):
        return (dp, CORES * ((z + ring - distance) % ring) + c)

    def remote(src, dst, send, recv, device):
        return pltpu.make_async_remote_copy(src_ref=src, dst_ref=dst, send_sem=send, recv_sem=recv, device_id=device, device_id_type=MESH)

    def part(block, chunk):
        first = pl.multiple_of(chunk * step, step)
        return wq.at[block, pl.ds(first, step)], wkv.at[block, chunk]

    own_first = pl.multiple_of(c * own, own)
    lane = own // 4
    x_loads = [pltpu.make_async_copy(x_hbm.at[pl.ds(i * lane, lane)], rows.at[pl.ds(own_first + i * lane, lane)], local_sem.at[i]) for i in range(4)]
    w_loads = []
    for i in range(QUARTERS):
        first = pl.multiple_of(((quarter + i) % QUARTERS) * (depth // QUARTERS), depth // QUARTERS)
        w_loads.append(pltpu.make_async_copy(wq_hbm.at[pl.ds(first, depth // QUARTERS)], wq.at[z, pl.ds(first, depth // QUARTERS)], local_sem.at[4 + i]))
    gain_load = pltpu.make_async_copy(gain_hbm, gain, local_sem.at[8])
    own_half = pl.ds(pl.multiple_of(c * piece, piece), piece)

    def columns(i):
        chunk = (HALVES * quarter + i) % CHUNKS
        return chunk, pl.ds(pl.multiple_of(chunk * step, step), step)

    def pair_load(source, i):
        chunk, span = columns(i)
        return pltpu.make_async_copy(source.at[:, span], wkv.at[z, chunk, own_half], local_sem.at[9 + i])

    def pair_copy(source, i):
        chunk, span = columns(i)
        return remote(source.at[:, span], wkv.at[z, chunk, own_half], pair_send.at[i], pair_recv.at[i], partner)

    def pair_arrival(i):
        chunk, span = columns(i)
        other_half = pl.ds(pl.multiple_of((1 - c) * piece, piece), piece)
        return remote(wk_hbm.at[:, span], wkv.at[z, chunk, other_half], pair_send.at[i], pair_recv.at[i], partner)

    w_loads[0].start()
    for load in x_loads:
        load.start()
    gain_load.start()

    @pl.when(c == 0)
    def _():
        for i in range(CHUNKS):
            pair_load(wk_hbm, i).start()

    @pl.when(c == 1)
    def _():
        for i in range(CHUNKS):
            pair_load(wv_hbm, i).start()

    for load in w_loads[1:]:
        load.start()

    barrier = pltpu.get_barrier_semaphore()
    peers = [x_peer, y_peer, partner] + [at_ring(r) for r in range(1, ring)]
    for peer in peers:
        pl.semaphore_signal(barrier, inc=1, device_id=peer, device_id_type=MESH)
    pl.semaphore_wait(barrier, len(peers))

    @pl.when(c == 0)
    def _():
        for i in range(CHUNKS):
            pair_copy(wv_hbm, i).start()

    @pl.when(c == 1)
    def _():
        for i in range(CHUNKS):
            pair_copy(wk_hbm, i).start()

    half_ring = ring // 2
    started = []

    def ring_send(direction, hop, half, kind):
        back = hop if direction == 0 else ring - hop
        block = (z + ring - back) % ring
        reference = part(block, HALVES * quarter + half)[kind]
        index = ((back * HALVES + half) * 2 + kind) if hop else ((direction * ring * HALVES + half) * 2 + kind)
        landed = (hop + 1) if direction == 0 else ring - hop - 1
        copy = remote(reference, reference, z_send.at[index], z_recv.at[(landed * HALVES + half) * 2 + kind], at_ring(ring - 1 if direction == 0 else 1))
        copy.start()
        started.append(copy)

    def reach(direction, half):
        return half_ring if direction == half else half_ring - 1

    def ring_arrival(direction, hop, half, kind):
        back = hop if direction == 0 else ring - hop
        block = (z + ring - back) % ring
        reference = part(block, HALVES * quarter + half)[kind]
        remote(reference, reference, z_send.at[0], z_recv.at[(back * HALVES + half) * 2 + kind], at_ring(1)).wait_recv()

    def ring_service(hop, kind, half):
        for direction in range(2):
            if hop <= reach(direction, half):
                ring_arrival(direction, hop, half, kind)
                if hop < reach(direction, half):
                    ring_send(direction, hop, half, kind)

    def square_copy(r, lane_index, chunk, kind, device):
        block = (z + ring - r) % ring
        reference = part(block, chunk)[kind]
        index = (r * 6 + lane_index) * 2 + kind
        return remote(reference, reference, xy_send.at[index], xy_recv.at[index], device)

    def square_send(r, kind, half):
        for base, device in ((0, x_peer), (2, y_peer)):
            copy = square_copy(r, base + half, HALVES * quarter + half, kind, device)
            copy.start()
            started.append(copy)

    def square_forward(r, kind, half):
        base, chunk, device = ((0, HALVES * quarter_x, y_peer), (2, HALVES * quarter_y, x_peer))[half]
        square_copy(r, base + half, chunk + half, kind, device).wait_recv()
        copy = square_copy(r, 4 + half, chunk + half, kind, device)
        copy.start()
        started.append(copy)

    def square_rest(r, kind):
        square_copy(r, 1, HALVES * quarter_x + 1, kind, x_peer).wait_recv()
        square_copy(r, 2, HALVES * quarter_y, kind, y_peer).wait_recv()
        square_copy(r, 4, HALVES * quarter_d, kind, y_peer).wait_recv()
        square_copy(r, 5, HALVES * quarter_d + 1, kind, x_peer).wait_recv()

    def flatten(block):
        @pl.loop(0, CHUNKS)
        def _(i):
            span = pl.ds(pl.multiple_of(i * step, step), step)
            wflat[span, :] = wq[block, span].reshape(step, wflat.shape[1])

    def product(block, slot, kind, first):
        span = pl.ds(first, TILE)
        if kind == 0:
            q = jnp.dot(rows[span, :], wflat[...], preferred_element_type=jnp.float32)
            oq[slot, span] = q.reshape((TILE,) + oq.shape[2:]).astype(oq.dtype)
        else:
            kv = jnp.zeros((TILE, okv.shape[2]), jnp.float32)
            for i in range(CHUNKS):
                kv += lax.dot_general(rows[span, pl.ds(i * step, step)], wkv[block, i], (((1,), (1,)), ((), ())), preferred_element_type=jnp.float32)
            okv[slot, span] = kv.astype(okv.dtype)

    def out_rows(block, first, count):
        return pl.ds(pl.multiple_of(block * chip_rows + first, TILE), count)

    def out_copy(r, kind, first, count):
        span, target = pl.ds(first, count), out_rows(z, first, count)
        if kind == 0:
            return remote(oq.at[r, span], q_out.at[target], oq_send.at[r], oq_recv.at[r], at_ring(r))
        return remote(okv.at[r, span], kv_out.at[c, target], okv_send.at[r], okv_recv.at[r], at_ring(r))

    def multiply(r, kind):
        block = (z + ring - r) % ring
        if kind == 0:
            flatten(block)

        @pl.loop(0, tiles)
        def _(t):
            first = pl.multiple_of(t * TILE, TILE)
            product(block, r, kind, first)
            if r:
                out_copy(r, kind, first, TILE).start()

    def keep_copy(kind):
        target = out_rows(z, 0, chip_rows)
        source, kept = ((oq.at[0], q_out.at[target]), (okv.at[0], kv_out.at[c, target]))[kind]
        return pltpu.make_async_copy(source, kept, keep_sem.at[kind])

    def hand_over(r, source):
        target = out_rows((z + r) % ring, 0, chip_rows)
        return remote(source, kv_out.at[c, target], fw_send.at[r], fw_recv.at[r], partner)

    def hand_arrival(r):
        target = out_rows((z + r) % ring, 0, chip_rows)
        return remote(okv.at[0], kv_out.at[1 - c, target], fw_send.at[r], fw_recv.at[r], partner)

    def relay(r):
        target = out_rows((z + r) % ring, 0, chip_rows)
        remote(okv.at[r], kv_out.at[c, target], okv_send.at[r], okv_recv.at[r], at_ring(r)).wait_recv()
        hand_over(r, kv_out.at[c, target]).start()

    for i in range(CHUNKS):
        pair_load(wk_hbm, i).wait()
    for half in range(HALVES):
        pair_arrival(half).wait_recv()
        for direction in range(2):
            ring_send(direction, 0, half, 1)
    w_loads[0].wait()
    for half in range(HALVES):
        for direction in range(2):
            ring_send(direction, 0, half, 0)
    gain_load.wait()

    def row_copy(i, core):
        span = pl.ds(pl.multiple_of(core * own + i * lane, lane), lane)
        return remote(rows.at[span], rows.at[span], x_send.at[i], x_recv.at[i], partner)

    def norm(i):
        x_loads[i].wait()

        @pl.loop(0, lane // NORM_ROWS)
        def _(n):
            span = pl.ds(pl.multiple_of(own_first + i * lane + n * NORM_ROWS, NORM_ROWS), NORM_ROWS)
            wide = rows[span, :].astype(jnp.float32)
            mean_sq = jnp.mean(wide * wide, axis=-1, keepdims=True)
            rows[span, :] = (wide * lax.rsqrt(mean_sq + EPSILON) * gain[...]).astype(rows.dtype)

        row_copy(i, c).start()

    normed = 0
    rows_complete = False
    for action, r, kind, half in SCHEDULE:
        if action in (MULTIPLY, OWN) and not rows_complete:
            rows_complete = True
            for i in range(4):
                row_copy(i, 1 - c).wait_recv()
        if action == ARRIVE:
            ring_service(r, kind, half)
        elif action == SPREAD:
            square_send(r, kind, half)
        elif action == FORWARD:
            square_forward(r, kind, half)
        elif action == MULTIPLY:
            square_rest(r, kind)
            multiply(r, kind)
        elif action == HAND_OVER:
            relay(r)
        elif action == NORM:
            norm(normed)
            normed += 1
        elif kind == 0:
            for load in w_loads[1:]:
                load.wait()
            multiply(0, 0)
            keep_copy(0).start()
        else:
            for i in range(HALVES, CHUNKS):
                pair_arrival(i).wait_recv()
            multiply(0, 1)
            keep_copy(1).start()
            hand_over(0, okv.at[0]).start()

    others = range(1, ring)
    for r in others:
        target = out_rows((z + r) % ring, 0, chip_rows)
        remote(oq.at[r], q_out.at[target], oq_send.at[r], oq_recv.at[r], at_ring(r)).wait_recv()
    for r in range(ring):
        hand_arrival(r).wait_recv()

    for kind in range(2):
        keep_copy(kind).wait()
    for copy in started:
        copy.wait_send()
    for r in others:
        for kind in range(2):
            out_copy(r, kind, 0, chip_rows).wait_send()
    for r in range(ring):
        hand_over(r, okv.at[0]).wait_send()
    for i in range(4):
        row_copy(i, c).wait_send()
    for i in range(CHUNKS):
        pair_copy(wk_hbm, i).wait_send()


def solution(mesh):
    ring = mesh.shape["tp"] // CORES
    side = math.isqrt(mesh.shape["dp"])
    assert side * side == mesh.shape["dp"] and side % 2 == 0

    def local_step(x_rows, norm_gain, w_q, w_k, w_v):
        own, depth = x_rows.shape
        heads, width = w_q.shape[1:]
        piece = w_k.shape[1]
        assert piece * CORES == width
        tokens, chip_rows, step = own * CORES * ring, own * CORES, depth // CHUNKS
        dma = pltpu.SemaphoreType.DMA
        bf16 = x_rows.dtype
        q_out, kv_out = pl.pallas_call(
            functools.partial(kernel, ring, side),
            out_shape=(
                jax.ShapeDtypeStruct((tokens, heads, width), bf16),
                jax.ShapeDtypeStruct((CORES, tokens, width), bf16),
            ),
            in_specs=[pl.BlockSpec(memory_space=pl.ANY)] * 5,
            out_specs=(pl.BlockSpec(memory_space=pl.ANY),) * 2,
            scratch_shapes=[
                pltpu.VMEM((chip_rows, depth), bf16),
                pltpu.VMEM((1, depth), jnp.float32),
                pltpu.VMEM((ring, depth, heads, width), bf16),
                pltpu.VMEM((ring, CHUNKS, width, step), bf16),
                pltpu.VMEM((depth, heads * width), bf16),
                pltpu.VMEM((ring, chip_rows, heads, width), bf16),
                pltpu.VMEM((ring, chip_rows, width), bf16),
                dma((9 + CHUNKS,)),
                dma((4,)), dma((4,)),
                dma((CHUNKS,)), dma((CHUNKS,)),
                dma((2 * ring * HALVES * 2,)), dma((ring * HALVES * 2,)),
                dma((ring * 6 * 2,)), dma((ring * 6 * 2,)),
                dma((ring,)), dma((ring,)), dma((ring,)), dma((ring,)),
                dma((ring,)), dma((ring,)),
                dma((2,)),
            ],
            compiler_params=pltpu.CompilerParams(collective_id=0, has_side_effects=True, vmem_limit_bytes=56 * 1024 * 1024),
        )(x_rows, norm_gain.reshape(1, depth), w_q, w_k.T, w_v.T)
        return q_out, kv_out[0][:, None, :], kv_out[1][:, None, :]

    return jax.shard_map(local_step, mesh=mesh, in_specs=(P(("dp", "tp"), None), P(None), P(None, "tp", None), P(None, "tp"), P(None, "tp")), out_specs=(P("dp", "tp", None), P("dp", "tp", None), P("dp", "tp", None)), check_vma=False)
```

```python
import functools
import math

import jax
import jax.numpy as jnp
from jax import lax
from jax.experimental import pallas as pl
from jax.experimental.pallas import tpu as pltpu
from jax.sharding import PartitionSpec as P

EPSILON = 1e-6
MESH = pl.DeviceIdType.MESH
CORES = 2
QUARTERS = 4
HALVES = 2
CHUNKS = QUARTERS * HALVES
TILE = 256
NORM_ROWS = 16

PAIRS, PRODUCTS, ROWS, HANDED = 2, 3, 5, 6

ARRIVE, SPREAD, FORWARD, MULTIPLY, HAND_OVER, NORM, OWN = range(7)
SCHEDULE = (
    (NORM, 0, 0, 0), (NORM, 0, 0, 0), (NORM, 0, 0, 0), (ARRIVE, 1, 1, 0), (SPREAD, 7, 1, 0),
    (NORM, 0, 0, 0), (ARRIVE, 1, 1, 1), (SPREAD, 7, 1, 1), (SPREAD, 1, 1, 0), (SPREAD, 1, 1, 1),
    (OWN, 0, 1, 0), (OWN, 0, 0, 0), (ARRIVE, 1, 0, 0), (FORWARD, 7, 1, 0), (FORWARD, 7, 1, 1),
    (FORWARD, 1, 1, 0), (ARRIVE, 1, 0, 1), (FORWARD, 1, 1, 1), (ARRIVE, 2, 1, 0), (SPREAD, 2, 1, 0),
    (MULTIPLY, 7, 1, 0), (ARRIVE, 2, 1, 1), (SPREAD, 2, 1, 1), (MULTIPLY, 1, 1, 0), (FORWARD, 2, 1, 0),
    (ARRIVE, 2, 0, 0), (SPREAD, 6, 0, 0), (FORWARD, 2, 1, 1), (ARRIVE, 2, 0, 1), (SPREAD, 6, 0, 1),
    (ARRIVE, 3, 1, 0), (SPREAD, 5, 1, 0), (FORWARD, 6, 0, 0), (MULTIPLY, 2, 1, 0), (HAND_OVER, 7, 1, 0),
    (FORWARD, 6, 0, 1), (ARRIVE, 3, 1, 1), (SPREAD, 5, 1, 1), (HAND_OVER, 1, 1, 0), (FORWARD, 5, 1, 0),
    (ARRIVE, 3, 0, 0), (SPREAD, 3, 0, 0), (MULTIPLY, 6, 0, 0), (ARRIVE, 3, 0, 1), (FORWARD, 5, 1, 1),
    (SPREAD, 3, 0, 1), (ARRIVE, 4, 1, 0), (SPREAD, 4, 1, 0), (FORWARD, 3, 0, 0), (MULTIPLY, 5, 1, 0),
    (ARRIVE, 4, 0, 0), (HAND_OVER, 2, 1, 0), (FORWARD, 3, 0, 1), (ARRIVE, 4, 1, 1), (SPREAD, 4, 1, 1),
    (SPREAD, 5, 0, 0), (SPREAD, 5, 0, 1), (FORWARD, 4, 1, 0), (ARRIVE, 4, 0, 1), (SPREAD, 3, 1, 0),
    (MULTIPLY, 3, 0, 0), (FORWARD, 4, 1, 1), (SPREAD, 3, 1, 1), (SPREAD, 4, 0, 0), (FORWARD, 5, 0, 0),
    (SPREAD, 4, 0, 1), (FORWARD, 5, 0, 1), (FORWARD, 3, 1, 0), (MULTIPLY, 4, 1, 0), (FORWARD, 3, 1, 1),
    (SPREAD, 2, 0, 0), (HAND_OVER, 5, 1, 0), (FORWARD, 4, 0, 0), (SPREAD, 2, 0, 1), (FORWARD, 4, 0, 1),
    (MULTIPLY, 5, 0, 0), (SPREAD, 6, 1, 0), (MULTIPLY, 3, 1, 0), (SPREAD, 6, 1, 1), (FORWARD, 2, 0, 0),
    (HAND_OVER, 4, 1, 0), (SPREAD, 1, 0, 0), (SPREAD, 1, 0, 1), (FORWARD, 2, 0, 1), (MULTIPLY, 4, 0, 0),
    (FORWARD, 6, 1, 0), (FORWARD, 6, 1, 1), (SPREAD, 7, 0, 0), (HAND_OVER, 3, 1, 0), (SPREAD, 7, 0, 1),
    (FORWARD, 1, 0, 0), (FORWARD, 1, 0, 1), (MULTIPLY, 2, 0, 0), (MULTIPLY, 6, 1, 0), (FORWARD, 7, 0, 0),
    (FORWARD, 7, 0, 1), (MULTIPLY, 1, 0, 0), (MULTIPLY, 7, 0, 0), (HAND_OVER, 6, 1, 0),
)


def kernel(ring, side, x_hbm, gain_hbm, wq_hbm, wk_hbm, wv_hbm, q_out, kv_out,
           rows, gain, wq, wkv, wflat, oq, okv,
           local_sem, send_sem, recv_sem, z_recv, xy_recv, okv_recv, keep_sem):
    dp, tp = lax.axis_index("dp"), lax.axis_index("tp")
    z, c = tp // CORES, tp % CORES
    grid_x, grid_y = dp // side, dp % side
    odd_x, odd_y = grid_x % 2, grid_y % 2
    quarter = 2 * odd_x + odd_y
    quarter_x, quarter_y, quarter_d = 2 * (1 - odd_x) + odd_y, 2 * odd_x + 1 - odd_y, 3 - quarter
    x_peer = (dp + side * (1 - 2 * odd_x), tp)
    y_peer = (dp + 1 - 2 * odd_y, tp)
    partner = (dp, tp + 1 - 2 * c)

    own, depth = x_hbm.shape
    chip_rows = CORES * own
    step = depth // CHUNKS
    piece = wk_hbm.shape[0]
    tiles = chip_rows // TILE

    def at_ring(distance):
        return (dp, CORES * ((z + ring - distance) % ring) + c)

    def remote(src, dst, send, recv, device):
        return pltpu.make_async_remote_copy(src_ref=src, dst_ref=dst, send_sem=send, recv_sem=recv, device_id=device, device_id_type=MESH)

    def part(block, chunk):
        first = pl.multiple_of(chunk * step, step)
        return wq.at[block, pl.ds(first, step)], wkv.at[block, chunk]

    own_first = pl.multiple_of(c * own, own)
    lane = own // 4
    x_loads = [pltpu.make_async_copy(x_hbm.at[pl.ds(i * lane, lane)], rows.at[pl.ds(own_first + i * lane, lane)], local_sem.at[i]) for i in range(4)]
    w_loads = []
    for i in range(QUARTERS):
        first = pl.multiple_of(((quarter + i) % QUARTERS) * (depth // QUARTERS), depth // QUARTERS)
        w_loads.append(pltpu.make_async_copy(wq_hbm.at[pl.ds(first, depth // QUARTERS)], wq.at[z, pl.ds(first, depth // QUARTERS)], local_sem.at[4 + min(i, 1)]))
    gain_load = pltpu.make_async_copy(gain_hbm, gain, local_sem.at[6])
    own_half = pl.ds(pl.multiple_of(c * piece, piece), piece)

    def columns(i):
        chunk = (HALVES * quarter + i) % CHUNKS
        return chunk, pl.ds(pl.multiple_of(chunk * step, step), step)

    def pair_load(source, i):
        chunk, span = columns(i)
        return pltpu.make_async_copy(source.at[:, span], wkv.at[z, chunk, own_half], local_sem.at[7])

    def pair_copy(source, i):
        chunk, span = columns(i)
        return remote(source.at[:, span], wkv.at[z, chunk, own_half], send_sem.at[PAIRS], recv_sem.at[3], partner)

    def pair_wait():
        pieces = wkv.at[z, :, own_half]
        remote(pieces, pieces, send_sem.at[PAIRS], recv_sem.at[3], partner).wait_recv()

    w_loads[0].start()
    for load in x_loads:
        load.start()
    gain_load.start()

    @pl.when(c == 0)
    def _():
        for i in range(CHUNKS):
            pair_load(wk_hbm, i).start()

    @pl.when(c == 1)
    def _():
        for i in range(CHUNKS):
            pair_load(wv_hbm, i).start()

    for load in w_loads[1:]:
        load.start()

    barrier = pltpu.get_barrier_semaphore()
    above, below = CORES * ((z + 1) % ring), CORES * ((z + ring - 1) % ring)
    peers = [x_peer, y_peer, partner] + [at_ring(r) for r in range(1, ring)] + [(dp, above + 1 - c), (dp, below + 1 - c)]
    for peer in peers:
        pl.semaphore_signal(barrier, inc=1, device_id=peer, device_id_type=MESH)
    pl.semaphore_wait(barrier, len(peers))

    def pair_start():
        @pl.when(c == 0)
        def _():
            for i in range(CHUNKS):
                pair_copy(wv_hbm, i).start()

        @pl.when(c == 1)
        def _():
            for i in range(CHUNKS):
                pair_copy(wk_hbm, i).start()

    half_ring = ring // 2

    def ring_send(direction, hop, half, kind):
        back = hop if direction == 0 else ring - hop
        block = (z + ring - back) % ring
        reference = part(block, HALVES * quarter + half)[kind]
        landed = (hop + 1) if direction == 0 else ring - hop - 1
        copy = remote(reference, reference, send_sem.at[kind], z_recv.at[(landed * HALVES + half) * 2 + kind], at_ring(ring - 1 if direction == 0 else 1))
        copy.start()

    def reach(direction, half):
        return half_ring if direction == half else half_ring - 1

    def key_value_start(half):
        chunk, span = columns(half)
        for direction in range(2):
            landed = 1 if direction == 0 else ring - 1
            for core, source in enumerate((wk_hbm, wv_hbm)):
                device = (dp, CORES * ((z + landed) % ring) + core)
                remote(source.at[:, span], wkv.at[z, chunk, own_half], send_sem.at[1], z_recv.at[(landed * HALVES + half) * 2 + 1], device).start()

    def ring_arrival(direction, hop, half, kind):
        back = hop if direction == 0 else ring - hop
        block = (z + ring - back) % ring
        reference = part(block, HALVES * quarter + half)[kind]
        remote(reference, reference, send_sem.at[kind], z_recv.at[(back * HALVES + half) * 2 + kind], at_ring(1)).wait_recv()

    def ring_service(hop, kind, half):
        for direction in range(2):
            if hop <= reach(direction, half):
                ring_arrival(direction, hop, half, kind)
                if hop < reach(direction, half):
                    ring_send(direction, hop, half, kind)

    def square_copy(r, lane_index, chunk, kind, device):
        block = (z + ring - r) % ring
        reference = part(block, chunk)[kind]
        index = (r * 3 + {0: 0, 3: 1}.get(lane_index, 2)) * 2 + kind
        return remote(reference, reference, send_sem.at[kind], xy_recv.at[index], device)

    def square_send(r, kind, half):
        for base, device in ((0, x_peer), (2, y_peer)):
            square_copy(r, base + half, HALVES * quarter + half, kind, device).start()

    def square_forward(r, kind, half):
        lane_index, chunk, device = ((0, HALVES * quarter_x, y_peer), (3, HALVES * quarter_y + 1, x_peer))[half]
        square_copy(r, lane_index, chunk, kind, device).wait_recv()
        square_copy(r, 4 + half, chunk, kind, device).start()

    def square_rest(r, kind):
        block = (z + ring - r) % ring
        four = (wq.at[block, pl.ds(0, 4 * step)], wkv.at[block, pl.ds(0, 4)])[kind]
        remote(four, four, send_sem.at[kind], xy_recv.at[(r * 3 + 2) * 2 + kind], x_peer).wait_recv()

    def flatten(block):
        @pl.loop(0, CHUNKS)
        def _(i):
            span = pl.ds(pl.multiple_of(i * step, step), step)
            wflat[span, :] = wq[block, span].reshape(step, wflat.shape[1])

    def product(block, slot, kind, first):
        span = pl.ds(first, TILE)
        if kind == 0:
            q = jnp.dot(rows[span, :], wflat[...], preferred_element_type=jnp.float32)
            oq[slot, span] = q.reshape((TILE,) + oq.shape[2:]).astype(oq.dtype)
        else:
            kv = jnp.zeros((TILE, okv.shape[2]), jnp.float32)
            for i in range(CHUNKS):
                kv += lax.dot_general(rows[span, pl.ds(i * step, step)], wkv[block, i], (((1,), (1,)), ((), ())), preferred_element_type=jnp.float32)
            okv[slot, span] = kv.astype(okv.dtype)

    def out_rows(block, first, count):
        return pl.ds(pl.multiple_of(block * chip_rows + first, TILE), count)

    def out_copy(r, kind, first, count):
        span, target = pl.ds(first, count), out_rows(z, first, count)
        if kind == 0:
            return remote(oq.at[r, span], q_out.at[target], send_sem.at[PRODUCTS], recv_sem.at[0], at_ring(r))
        return remote(okv.at[r, span], kv_out.at[c, target], send_sem.at[PRODUCTS + 1], okv_recv.at[r], at_ring(r))

    def multiply(r, kind):
        block = (z + ring - r) % ring
        if kind == 0:
            flatten(block)

        @pl.loop(0, tiles)
        def _(t):
            first = pl.multiple_of(t * TILE, TILE)
            product(block, r, kind, first)
            if r:
                out_copy(r, kind, first, TILE).start()

    def keep_copy(kind):
        target = out_rows(z, 0, chip_rows)
        source, kept = ((oq.at[0], q_out.at[target]), (okv.at[0], kv_out.at[c, target]))[kind]
        return pltpu.make_async_copy(source, kept, keep_sem.at[kind])

    def hand_over(r, source):
        target = out_rows((z + r) % ring, 0, chip_rows)
        return remote(source, kv_out.at[c, target], send_sem.at[HANDED], recv_sem.at[1], partner)

    def relay(r):
        target = out_rows((z + r) % ring, 0, chip_rows)
        remote(okv.at[r], kv_out.at[c, target], send_sem.at[PRODUCTS + 1], okv_recv.at[r], at_ring(r)).wait_recv()
        hand_over(r, kv_out.at[c, target]).start()

    for half in range(HALVES):
        key_value_start(half)
    w_loads[0].wait()
    for half in range(HALVES):
        for direction in range(2):
            ring_send(direction, 0, half, 0)
    pair_start()
    for i in range(CHUNKS):
        pair_load(wk_hbm, i).wait()
    gain_load.wait()

    def row_copy(i, core):
        span = pl.ds(pl.multiple_of(core * own + i * lane, lane), lane)
        return remote(rows.at[span], rows.at[span], send_sem.at[ROWS], recv_sem.at[2], partner)

    def half_rows(core):
        span = pl.ds(pl.multiple_of(core * own, own), own)
        return remote(rows.at[span], rows.at[span], send_sem.at[ROWS], recv_sem.at[2], partner)

    def norm(i):
        x_loads[i].wait()

        @pl.loop(0, lane // NORM_ROWS)
        def _(n):
            span = pl.ds(pl.multiple_of(own_first + i * lane + n * NORM_ROWS, NORM_ROWS), NORM_ROWS)
            wide = rows[span, :].astype(jnp.float32)
            mean_sq = jnp.mean(wide * wide, axis=-1, keepdims=True)
            rows[span, :] = (wide * lax.rsqrt(mean_sq + EPSILON) * gain[...]).astype(rows.dtype)

        row_copy(i, c).start()

    normed = 0
    rows_complete = False
    for action, r, kind, half in SCHEDULE:
        if action in (MULTIPLY, OWN) and not rows_complete:
            rows_complete = True
            half_rows(1 - c).wait_recv()
        if action == ARRIVE:
            ring_service(r, kind, half)
        elif action == SPREAD:
            square_send(r, kind, half)
        elif action == FORWARD:
            square_forward(r, kind, half)
        elif action == MULTIPLY:
            square_rest(r, kind)
            multiply(r, kind)
        elif action == HAND_OVER:
            relay(r)
        elif action == NORM:
            norm(normed)
            normed += 1
        elif kind == 0:
            for load in w_loads[1:]:
                load.wait()
            multiply(0, 0)
            keep_copy(0).start()
        else:
            pair_wait()
            multiply(0, 1)
            keep_copy(1).start()
            hand_over(0, okv.at[0]).start()

    for kind in range(2):
        keep_copy(kind).wait()

    def whole(source, target, send, recv):
        return remote(source, target, send_sem.at[send], recv_sem.at[recv], partner)

    others = ring - 1
    products = q_out.at[pl.ds(0, others * chip_rows)]
    whole(products, products, PRODUCTS, 0).wait_recv()
    heads = kv_out.at[1 - c]
    whole(heads, heads, HANDED, 1).wait()
    half_rows(c).wait_send()
    for kind, weights in enumerate((wq, wkv)):
        sent = weights.at[pl.ds(0, others)]
        whole(sent, sent, kind, 0).wait_send()
    for kind, buffer in enumerate((oq, okv)):
        sent = buffer.at[pl.ds(0, others)]
        whole(sent, sent, PRODUCTS + kind, 0).wait_send()
    pieces = wkv.at[z, :, own_half]
    whole(pieces, pieces, PAIRS, 0).wait_send()


def flush(q_ref, kv_ref, q_out, k_out, v_out, sem):
    copies = [pltpu.make_async_copy(source, target, sem.at[i]) for i, (source, target) in enumerate(((q_ref, q_out), (kv_ref.at[0], k_out), (kv_ref.at[1], v_out)))]
    for copy in copies:
        copy.start()
    for copy in copies:
        copy.wait()


def solution(mesh):
    ring = mesh.shape["tp"] // CORES
    side = math.isqrt(mesh.shape["dp"])
    assert side * side == mesh.shape["dp"] and side % 2 == 0

    def local_step(x_rows, norm_gain, w_q, w_k, w_v):
        own, depth = x_rows.shape
        heads, width = w_q.shape[1:]
        piece = w_k.shape[1]
        assert piece * CORES == width
        tokens, chip_rows, step = own * CORES * ring, own * CORES, depth // CHUNKS
        dma = pltpu.SemaphoreType.DMA
        bf16 = x_rows.dtype
        q_out, kv_out = pl.pallas_call(
            functools.partial(kernel, ring, side),
            out_shape=(
                jax.ShapeDtypeStruct((tokens, heads, width), bf16),
                jax.ShapeDtypeStruct((CORES, tokens, width), bf16),
            ),
            in_specs=[pl.BlockSpec(memory_space=pltpu.HBM)] * 5,
            out_specs=(pl.BlockSpec(memory_space=pl.ANY),) * 2,
            scratch_shapes=[
                pltpu.VMEM((chip_rows, depth), bf16),
                pltpu.VMEM((1, depth), jnp.float32),
                pltpu.VMEM((ring, depth, heads, width), bf16),
                pltpu.VMEM((ring, CHUNKS, width, step), bf16),
                pltpu.VMEM((depth, heads * width), bf16),
                pltpu.VMEM((ring, chip_rows, heads, width), bf16),
                pltpu.VMEM((ring, chip_rows, width), bf16),
                dma((8,)), dma((HANDED + 1,)), dma((4,)),
                dma((ring * HALVES * 2,)), dma((ring * 3 * 2,)), dma((ring,)), dma((2,)),
            ],
            compiler_params=pltpu.CompilerParams(collective_id=0, has_side_effects=True, vmem_limit_bytes=42 * 1024 * 1024),
        )(*(pltpu.with_memory_space_constraint(a, pltpu.HBM) for a in (x_rows, norm_gain.reshape(1, depth), w_q, w_k.T, w_v.T)))
        head = jax.ShapeDtypeStruct((tokens, width), bf16)
        q_out, k_out, v_out = pl.pallas_call(
            flush,
            out_shape=(jax.ShapeDtypeStruct((tokens, heads, width), bf16), head, head),
            in_specs=[pl.BlockSpec(memory_space=pl.ANY)] * 2,
            out_specs=(pl.BlockSpec(memory_space=pl.ANY),) * 3,
            scratch_shapes=[dma((3,))],
            compiler_params=pltpu.CompilerParams(vmem_limit_bytes=1024 * 1024),
        )(q_out, kv_out)
        return q_out, k_out[:, None, :], v_out[:, None, :]

    return jax.shard_map(local_step, mesh=mesh, in_specs=(P(("dp", "tp"), None), P(None), P(None, "tp", None), P(None, "tp"), P(None, "tp")), out_specs=(P("dp", "tp", None), P("dp", "tp", None), P("dp", "tp", None)), check_vma=False)
```

```python
import functools
import math

import jax
import jax.numpy as jnp
from jax import lax
from jax.experimental import pallas as pl
from jax.experimental.pallas import tpu as pltpu
from jax.sharding import PartitionSpec as P

EPSILON = 1e-6
MESH = pl.DeviceIdType.MESH
CORES = 2
QUARTERS = 4
HALVES = 2
CHUNKS = QUARTERS * HALVES
TILE = 128
NORM_ROWS = 16

PAIRS, PRODUCTS, ROWS, HANDED = 2, 3, 5, 6

ARRIVE, SPREAD, FORWARD, MULTIPLY, HAND_OVER, NORM, OWN = range(7)
SCHEDULE = (
    (ARRIVE, 1, 1, 0), (SPREAD, 7, 1, 0), (NORM, 0, 0, 0), (ARRIVE, 1, 1, 1), (SPREAD, 1, 1, 1),
    (SPREAD, 7, 1, 1), (SPREAD, 1, 1, 0), (NORM, 0, 0, 0), (FORWARD, 1, 1, 1), (FORWARD, 7, 1, 0),
    (FORWARD, 7, 1, 1), (ARRIVE, 1, 0, 0), (ARRIVE, 1, 0, 1), (FORWARD, 1, 1, 0), (ARRIVE, 2, 1, 0),
    (SPREAD, 6, 1, 0), (ARRIVE, 2, 1, 1), (SPREAD, 2, 1, 0), (SPREAD, 2, 1, 1), (ARRIVE, 2, 0, 0),
    (SPREAD, 6, 0, 0), (ARRIVE, 2, 0, 1), (SPREAD, 6, 0, 1), (NORM, 0, 0, 0), (NORM, 0, 0, 0),
    (FORWARD, 6, 0, 0), (FORWARD, 2, 1, 0), (ARRIVE, 3, 1, 1), (SPREAD, 3, 1, 1), (ARRIVE, 3, 1, 0),
    (FORWARD, 2, 1, 1), (FORWARD, 6, 0, 1), (ARRIVE, 3, 0, 0), (ARRIVE, 3, 0, 1), (SPREAD, 3, 0, 1),
    (SPREAD, 3, 0, 0), (SPREAD, 5, 1, 1), (SPREAD, 5, 1, 0), (MULTIPLY, 1, 1, 0), (MULTIPLY, 6, 0, 0),
    (ARRIVE, 4, 0, 1), (MULTIPLY, 2, 1, 0), (FORWARD, 3, 0, 0), (FORWARD, 3, 0, 1), (FORWARD, 5, 1, 1),
    (MULTIPLY, 7, 1, 0), (FORWARD, 5, 1, 0), (ARRIVE, 4, 1, 0), (SPREAD, 5, 0, 0), (ARRIVE, 4, 1, 1),
    (OWN, 0, 1, 0), (MULTIPLY, 3, 0, 0), (SPREAD, 4, 1, 0), (SPREAD, 5, 0, 1), (ARRIVE, 4, 0, 0),
    (SPREAD, 4, 1, 1), (MULTIPLY, 5, 1, 0), (SPREAD, 3, 1, 0), (FORWARD, 4, 1, 0), (SPREAD, 6, 1, 1),
    (FORWARD, 5, 0, 0), (FORWARD, 4, 1, 1), (FORWARD, 5, 0, 1), (FORWARD, 6, 1, 0), (FORWARD, 6, 1, 1),
    (MULTIPLY, 4, 1, 0), (SPREAD, 4, 0, 1), (HAND_OVER, 1, 1, 0), (FORWARD, 3, 1, 0), (FORWARD, 3, 1, 1),
    (MULTIPLY, 6, 1, 0), (SPREAD, 4, 0, 0), (FORWARD, 4, 0, 1), (SPREAD, 2, 0, 1), (MULTIPLY, 3, 1, 0),
    (MULTIPLY, 5, 0, 0), (FORWARD, 4, 0, 0), (SPREAD, 2, 0, 0), (HAND_OVER, 7, 1, 0), (SPREAD, 1, 0, 0),
    (MULTIPLY, 4, 0, 0), (HAND_OVER, 3, 1, 0), (FORWARD, 2, 0, 0), (FORWARD, 2, 0, 1), (SPREAD, 1, 0, 1),
    (SPREAD, 7, 0, 1), (OWN, 0, 0, 0), (SPREAD, 7, 0, 0), (MULTIPLY, 2, 0, 0), (FORWARD, 1, 0, 0),
    (HAND_OVER, 2, 1, 0), (FORWARD, 1, 0, 1), (FORWARD, 7, 0, 0), (FORWARD, 7, 0, 1), (HAND_OVER, 5, 1, 0),
    (HAND_OVER, 4, 1, 0), (MULTIPLY, 1, 0, 0), (MULTIPLY, 7, 0, 0), (HAND_OVER, 6, 1, 0),
)


def kernel(ring, side, x_hbm, gain_hbm, wq_hbm, wk_hbm, wv_hbm, q_out, kv_out,
           rows, gain, wq, wkv, wflat, oq, okv,
           local_sem, send_sem, recv_sem, z_recv, xy_recv, okv_recv, keep_sem):
    dp, tp = lax.axis_index("dp"), lax.axis_index("tp")
    z, c = tp // CORES, tp % CORES
    grid_x, grid_y = dp // side, dp % side
    odd_x, odd_y = grid_x % 2, grid_y % 2
    quarter = 2 * odd_x + odd_y
    quarter_x, quarter_y, quarter_d = 2 * (1 - odd_x) + odd_y, 2 * odd_x + 1 - odd_y, 3 - quarter
    x_peer = (dp + side * (1 - 2 * odd_x), tp)
    y_peer = (dp + 1 - 2 * odd_y, tp)
    partner = (dp, tp + 1 - 2 * c)

    own, depth = x_hbm.shape
    chip_rows = CORES * own
    step = depth // CHUNKS
    piece = wk_hbm.shape[0]
    tiles = chip_rows // TILE

    def at_ring(distance):
        return (dp, CORES * ((z + ring - distance) % ring) + c)

    def remote(src, dst, send, recv, device):
        return pltpu.make_async_remote_copy(src_ref=src, dst_ref=dst, send_sem=send, recv_sem=recv, device_id=device, device_id_type=MESH)

    def part(block, chunk):
        first = pl.multiple_of(chunk * step, step)
        return wq.at[block, pl.ds(first, step)], wkv.at[block, chunk]

    barrier = pltpu.get_barrier_semaphore()
    above, below = CORES * ((z + 1) % ring), CORES * ((z + ring - 1) % ring)
    peers = [x_peer, y_peer, partner] + [at_ring(1), at_ring(ring - 1)] + [(dp, above + 1 - c), (dp, below + 1 - c)]
    for peer in peers:
        pl.semaphore_signal(barrier, inc=1, device_id=peer, device_id_type=MESH)

    own_first = pl.multiple_of(c * own, own)
    lane = own // 4
    x_loads = [pltpu.make_async_copy(x_hbm.at[pl.ds(i * lane, lane)], rows.at[pl.ds(own_first + i * lane, lane)], local_sem.at[i]) for i in range(4)]
    w_loads = []
    for i in range(QUARTERS):
        first = pl.multiple_of(((quarter + i) % QUARTERS) * (depth // QUARTERS), depth // QUARTERS)
        w_loads.append(pltpu.make_async_copy(wq_hbm.at[pl.ds(first, depth // QUARTERS)], wq.at[z, pl.ds(first, depth // QUARTERS)], local_sem.at[4 + min(i, 1)]))
    gain_load = pltpu.make_async_copy(gain_hbm, gain, local_sem.at[6])
    own_half = pl.ds(pl.multiple_of(c * piece, piece), piece)

    def columns(i):
        chunk = (HALVES * quarter + i) % CHUNKS
        return chunk, pl.ds(pl.multiple_of(chunk * step, step), step)

    def pair_load(source, i):
        chunk, span = columns(i)
        return pltpu.make_async_copy(source.at[:, span], wkv.at[z, chunk, own_half], local_sem.at[7])

    def pair_copy(source, i):
        chunk, span = columns(i)
        return remote(source.at[:, span], wkv.at[z, chunk, own_half], send_sem.at[PAIRS], recv_sem.at[3], partner)

    def pair_wait():
        pieces = wkv.at[z, :, own_half]
        remote(pieces, pieces, send_sem.at[PAIRS], recv_sem.at[3], partner).wait_recv()

    w_loads[0].start()
    for load in x_loads:
        load.start()
    gain_load.start()

    @pl.when(c == 0)
    def _():
        for i in range(CHUNKS):
            pair_load(wk_hbm, i).start()

    @pl.when(c == 1)
    def _():
        for i in range(CHUNKS):
            pair_load(wv_hbm, i).start()

    for load in w_loads[1:]:
        load.start()

    pl.semaphore_wait(barrier, len(peers))

    def pair_start():
        @pl.when(c == 0)
        def _():
            for i in range(CHUNKS):
                pair_copy(wv_hbm, i).start()

        @pl.when(c == 1)
        def _():
            for i in range(CHUNKS):
                pair_copy(wk_hbm, i).start()

    half_ring = ring // 2

    def ring_send(direction, hop, half, kind):
        back = hop if direction == 0 else ring - hop
        block = (z + ring - back) % ring
        reference = part(block, HALVES * quarter + half)[kind]
        landed = (hop + 1) if direction == 0 else ring - hop - 1
        copy = remote(reference, reference, send_sem.at[kind], z_recv.at[(landed * HALVES + half) * 2 + kind], at_ring(ring - 1 if direction == 0 else 1))
        copy.start()

    def reach(direction, half):
        return half_ring if direction == half else half_ring - 1

    def key_value_start(half):
        chunk, span = columns(half)
        for direction in range(2):
            landed = 1 if direction == 0 else ring - 1
            for core, source in enumerate((wk_hbm, wv_hbm)):
                device = (dp, CORES * ((z + landed) % ring) + core)
                remote(source.at[:, span], wkv.at[z, chunk, own_half], send_sem.at[1], z_recv.at[(landed * HALVES + half) * 2 + 1], device).start()

    def query_start(half):
        span = pl.ds(pl.multiple_of((HALVES * quarter + half) * step, step), step)
        for direction in range(2):
            landed = 1 if direction == 0 else ring - 1
            remote(wq_hbm.at[span], wq.at[z, span], send_sem.at[0], z_recv.at[(landed * HALVES + half) * 2], at_ring(ring - landed)).start()

    def ring_arrival(direction, hop, half, kind):
        back = hop if direction == 0 else ring - hop
        block = (z + ring - back) % ring
        reference = part(block, HALVES * quarter + half)[kind]
        remote(reference, reference, send_sem.at[kind], z_recv.at[(back * HALVES + half) * 2 + kind], at_ring(1)).wait_recv()

    def ring_service(hop, kind, half):
        for direction in range(2):
            if hop <= reach(direction, half):
                ring_arrival(direction, hop, half, kind)
                if hop < reach(direction, half):
                    ring_send(direction, hop, half, kind)

    def square_copy(r, lane_index, chunk, kind, device):
        block = (z + ring - r) % ring
        reference = part(block, chunk)[kind]
        index = (r * 3 + {0: 0, 3: 1}.get(lane_index, 2)) * 2 + kind
        return remote(reference, reference, send_sem.at[kind], xy_recv.at[index], device)

    def square_send(r, kind, half):
        for base, device in ((0, x_peer), (2, y_peer)):
            square_copy(r, base + half, HALVES * quarter + half, kind, device).start()

    def square_forward(r, kind, half):
        lane_index, chunk, device = ((0, HALVES * quarter_x, y_peer), (3, HALVES * quarter_y + 1, x_peer))[half]
        square_copy(r, lane_index, chunk, kind, device).wait_recv()
        square_copy(r, 4 + half, chunk, kind, device).start()

    def square_rest(r, kind):
        block = (z + ring - r) % ring
        four = (wq.at[block, pl.ds(0, 4 * step)], wkv.at[block, pl.ds(0, 4)])[kind]
        remote(four, four, send_sem.at[kind], xy_recv.at[(r * 3 + 2) * 2 + kind], x_peer).wait_recv()

    def flatten(block):
        @pl.loop(0, CHUNKS)
        def _(i):
            span = pl.ds(pl.multiple_of(i * step, step), step)
            wflat[span, :] = wq[block, span].reshape(step, wflat.shape[1])

    def product(block, slot, kind, first):
        span = pl.ds(first, TILE)
        if kind == 0:
            q = jnp.dot(rows[span, :], wflat[...], preferred_element_type=jnp.float32)
            oq[slot, span] = q.reshape((TILE,) + oq.shape[2:]).astype(oq.dtype)
        else:
            kv = jnp.zeros((TILE, okv.shape[2]), jnp.float32)
            for i in range(CHUNKS):
                kv += lax.dot_general(rows[span, pl.ds(i * step, step)], wkv[block, i], (((1,), (1,)), ((), ())), preferred_element_type=jnp.float32)
            okv[slot, span] = kv.astype(okv.dtype)

    def out_rows(block, first, count):
        return pl.ds(pl.multiple_of(block * chip_rows + first, TILE), count)

    def out_copy(r, kind, first, count):
        span, target = pl.ds(first, count), out_rows(z, first, count)
        if kind == 0:
            return remote(oq.at[r, span], q_out.at[target], send_sem.at[PRODUCTS], recv_sem.at[0], at_ring(r))
        return remote(okv.at[r, span], kv_out.at[c, target], send_sem.at[PRODUCTS + 1], okv_recv.at[r], at_ring(r))

    def multiply(r, kind):
        block = (z + ring - r) % ring
        if kind == 0:
            flatten(block)

        @pl.loop(0, tiles)
        def _(t):
            first = pl.multiple_of(t * TILE, TILE)
            product(block, r, kind, first)
            if r:
                out_copy(r, kind, first, TILE).start()

    def keep_copy(kind):
        target = out_rows(z, 0, chip_rows)
        source, kept = ((oq.at[0], q_out.at[target]), (okv.at[0], kv_out.at[c, target]))[kind]
        return pltpu.make_async_copy(source, kept, keep_sem.at[kind])

    def hand_over(r, source):
        target = out_rows((z + r) % ring, 0, chip_rows)
        return remote(source, kv_out.at[c, target], send_sem.at[HANDED], recv_sem.at[1], partner)

    def relay(r):
        target = out_rows((z + r) % ring, 0, chip_rows)
        remote(okv.at[r], kv_out.at[c, target], send_sem.at[PRODUCTS + 1], okv_recv.at[r], at_ring(r)).wait_recv()
        hand_over(r, kv_out.at[c, target]).start()

    for half in range(HALVES):
        key_value_start(half)
    for half in range(HALVES):
        query_start(half)
    pair_start()
    for i in range(CHUNKS):
        pair_load(wk_hbm, i).wait()
    gain_load.wait()

    def row_copy(i, core):
        span = pl.ds(pl.multiple_of(core * own + i * lane, lane), lane)
        return remote(rows.at[span], rows.at[span], send_sem.at[ROWS], recv_sem.at[2], partner)

    def half_rows(core):
        span = pl.ds(pl.multiple_of(core * own, own), own)
        return remote(rows.at[span], rows.at[span], send_sem.at[ROWS], recv_sem.at[2], partner)

    def norm(i):
        x_loads[i].wait()

        @pl.loop(0, lane // NORM_ROWS)
        def _(n):
            span = pl.ds(pl.multiple_of(own_first + i * lane + n * NORM_ROWS, NORM_ROWS), NORM_ROWS)
            wide = rows[span, :].astype(jnp.float32)
            mean_sq = jnp.mean(wide * wide, axis=-1, keepdims=True)
            rows[span, :] = (wide * lax.rsqrt(mean_sq + EPSILON) * gain[...]).astype(rows.dtype)

        row_copy(i, c).start()

    normed = 0
    rows_complete = False
    for action, r, kind, half in SCHEDULE:
        if action in (MULTIPLY, OWN) and not rows_complete:
            rows_complete = True
            half_rows(1 - c).wait_recv()
        if action == ARRIVE:
            ring_service(r, kind, half)
        elif action == SPREAD:
            square_send(r, kind, half)
        elif action == FORWARD:
            square_forward(r, kind, half)
        elif action == MULTIPLY:
            square_rest(r, kind)
            multiply(r, kind)
        elif action == HAND_OVER:
            relay(r)
        elif action == NORM:
            norm(normed)
            normed += 1
        elif kind == 0:
            for load in w_loads:
                load.wait()
            multiply(0, 0)
            keep_copy(0).start()
        else:
            pair_wait()
            multiply(0, 1)
            keep_copy(1).start()
            hand_over(0, okv.at[0]).start()

    for kind in range(2):
        keep_copy(kind).wait()

    def whole(source, target, send, recv):
        return remote(source, target, send_sem.at[send], recv_sem.at[recv], partner)

    others = ring - 1
    products = q_out.at[pl.ds(0, others * chip_rows)]
    whole(products, products, PRODUCTS, 0).wait_recv()
    heads = kv_out.at[1 - c]
    whole(heads, heads, HANDED, 1).wait()
    half_rows(c).wait_send()
    for kind, weights in enumerate((wq, wkv)):
        sent = weights.at[pl.ds(0, others)]
        whole(sent, sent, kind, 0).wait_send()
    for kind, buffer in enumerate((oq, okv)):
        sent = buffer.at[pl.ds(0, others)]
        whole(sent, sent, PRODUCTS + kind, 0).wait_send()
    pieces = wkv.at[z, :, own_half]
    whole(pieces, pieces, PAIRS, 0).wait_send()


def flush(q_ref, kv_ref, q_out, k_out, v_out, sem):
    copies = [pltpu.make_async_copy(source, target, sem.at[i]) for i, (source, target) in enumerate(((q_ref, q_out), (kv_ref.at[0], k_out), (kv_ref.at[1], v_out)))]
    for copy in copies:
        copy.start()
    for copy in copies:
        copy.wait()


def solution(mesh):
    ring = mesh.shape["tp"] // CORES
    side = math.isqrt(mesh.shape["dp"])
    assert side * side == mesh.shape["dp"] and side % 2 == 0

    def local_step(x_rows, norm_gain, w_q, w_k, w_v):
        own, depth = x_rows.shape
        heads, width = w_q.shape[1:]
        piece = w_k.shape[1]
        assert piece * CORES == width
        tokens, chip_rows, step = own * CORES * ring, own * CORES, depth // CHUNKS
        dma = pltpu.SemaphoreType.DMA
        bf16 = x_rows.dtype
        q_out, kv_out = pl.pallas_call(
            functools.partial(kernel, ring, side),
            out_shape=(
                jax.ShapeDtypeStruct((tokens, heads, width), bf16),
                jax.ShapeDtypeStruct((CORES, tokens, width), bf16),
            ),
            in_specs=[pl.BlockSpec(memory_space=pltpu.HBM)] * 5,
            out_specs=(pl.BlockSpec(memory_space=pl.ANY),) * 2,
            scratch_shapes=[
                pltpu.VMEM((chip_rows, depth), bf16),
                pltpu.VMEM((1, depth), jnp.float32),
                pltpu.VMEM((ring, depth, heads, width), bf16),
                pltpu.VMEM((ring, CHUNKS, width, step), bf16),
                pltpu.VMEM((depth, heads * width), bf16),
                pltpu.VMEM((ring, chip_rows, heads, width), bf16),
                pltpu.VMEM((ring, chip_rows, width), bf16),
                dma((8,)), dma((HANDED + 1,)), dma((4,)),
                dma((ring * HALVES * 2,)), dma((ring * 3 * 2,)), dma((ring,)), dma((2,)),
            ],
            compiler_params=pltpu.CompilerParams(collective_id=0, has_side_effects=True, vmem_limit_bytes=42 * 1024 * 1024),
        )(*(pltpu.with_memory_space_constraint(a, pltpu.HBM) for a in (x_rows, norm_gain.reshape(1, depth), w_q, w_k.T, w_v.T)))
        head = jax.ShapeDtypeStruct((tokens, width), bf16)
        q_out, k_out, v_out = pl.pallas_call(
            flush,
            out_shape=(jax.ShapeDtypeStruct((tokens, heads, width), bf16), head, head),
            in_specs=[pl.BlockSpec(memory_space=pl.ANY)] * 2,
            out_specs=(pl.BlockSpec(memory_space=pl.ANY),) * 3,
            scratch_shapes=[dma((3,))],
            compiler_params=pltpu.CompilerParams(vmem_limit_bytes=1024 * 1024),
        )(q_out, kv_out)
        return q_out, k_out[:, None, :], v_out[:, None, :]

    return jax.shard_map(local_step, mesh=mesh, in_specs=(P(("dp", "tp"), None), P(None), P(None, "tp", None), P(None, "tp"), P(None, "tp")), out_specs=(P("dp", "tp", None), P("dp", "tp", None), P("dp", "tp", None)), check_vma=False)
```

```python
import functools
import math

import jax
import jax.numpy as jnp
from jax import lax
from jax.experimental import pallas as pl
from jax.experimental.pallas import tpu as pltpu
from jax.sharding import PartitionSpec as P

EPSILON = 1e-6
MESH = pl.DeviceIdType.MESH
CORES = 2
QUARTERS = 4
HALVES = 2
CHUNKS = QUARTERS * HALVES
TILE = 128
NORM_ROWS = 16

PAIRS, PRODUCTS, ROWS, HANDED = 2, 3, 5, 6

ARRIVE, SPREAD, FORWARD, MULTIPLY, HAND_OVER, NORM, OWN = range(7)
SCHEDULE = (
    (NORM, 0, 0, 0), (ARRIVE, 1, 1, 0), (SPREAD, 7, 1, 0), (ARRIVE, 1, 1, 1), (SPREAD, 1, 1, 0),
    (SPREAD, 7, 1, 1), (SPREAD, 1, 1, 1), (FORWARD, 1, 1, 0), (FORWARD, 7, 1, 0), (FORWARD, 7, 1, 1),
    (ARRIVE, 1, 0, 1), (FORWARD, 1, 1, 1), (ARRIVE, 2, 1, 0), (SPREAD, 2, 1, 0), (NORM, 0, 0, 0),
    (ARRIVE, 2, 1, 1), (SPREAD, 6, 1, 0), (NORM, 0, 0, 0), (SPREAD, 6, 1, 1), (ARRIVE, 1, 0, 0),
    (NORM, 0, 0, 0), (SPREAD, 2, 1, 1), (ARRIVE, 2, 0, 1), (SPREAD, 6, 0, 1), (FORWARD, 2, 1, 1),
    (ARRIVE, 3, 1, 0), (ARRIVE, 3, 1, 1), (SPREAD, 5, 1, 1), (ARRIVE, 2, 0, 0), (FORWARD, 2, 1, 0),
    (SPREAD, 5, 1, 0), (ARRIVE, 3, 0, 1), (SPREAD, 3, 0, 1), (MULTIPLY, 7, 1, 0), (FORWARD, 5, 1, 0),
    (FORWARD, 5, 1, 1), (MULTIPLY, 2, 1, 0), (ARRIVE, 3, 0, 0), (SPREAD, 3, 0, 0), (SPREAD, 6, 0, 0),
    (MULTIPLY, 1, 1, 0), (ARRIVE, 4, 1, 1), (FORWARD, 3, 0, 1), (MULTIPLY, 5, 1, 0), (ARRIVE, 4, 1, 0),
    (FORWARD, 6, 0, 1), (OWN, 0, 1, 0), (FORWARD, 3, 0, 0), (FORWARD, 6, 0, 0), (SPREAD, 4, 1, 1),
    (ARRIVE, 4, 0, 1), (ARRIVE, 4, 0, 0), (SPREAD, 5, 0, 1), (SPREAD, 4, 1, 0), (SPREAD, 3, 1, 1),
    (FORWARD, 6, 1, 0), (MULTIPLY, 3, 0, 0), (SPREAD, 4, 0, 1), (MULTIPLY, 6, 0, 0), (FORWARD, 6, 1, 1),
    (FORWARD, 4, 1, 0), (OWN, 0, 0, 0), (SPREAD, 3, 1, 0), (FORWARD, 4, 1, 1), (SPREAD, 5, 0, 0),
    (MULTIPLY, 6, 1, 0), (SPREAD, 4, 0, 0), (FORWARD, 3, 1, 1), (FORWARD, 3, 1, 0), (MULTIPLY, 4, 1, 0),
    (FORWARD, 5, 0, 1), (FORWARD, 5, 0, 0), (SPREAD, 7, 0, 0), (MULTIPLY, 3, 1, 0), (HAND_OVER, 7, 1, 0),
    (FORWARD, 4, 0, 0), (FORWARD, 4, 0, 1), (HAND_OVER, 1, 1, 0), (MULTIPLY, 5, 0, 0), (SPREAD, 2, 0, 1),
    (SPREAD, 2, 0, 0), (MULTIPLY, 4, 0, 0), (SPREAD, 1, 0, 1), (FORWARD, 2, 0, 0), (FORWARD, 2, 0, 1),
    (SPREAD, 1, 0, 0), (SPREAD, 7, 0, 1), (MULTIPLY, 2, 0, 0), (FORWARD, 1, 0, 1), (FORWARD, 1, 0, 0),
    (HAND_OVER, 6, 1, 0), (HAND_OVER, 4, 1, 0), (FORWARD, 7, 0, 1), (FORWARD, 7, 0, 0), (MULTIPLY, 1, 0, 0),
    (MULTIPLY, 7, 0, 0), (HAND_OVER, 5, 1, 0), (HAND_OVER, 3, 1, 0), (HAND_OVER, 2, 1, 0),
)


def kernel(ring, side, x_hbm, gain_hbm, wq_hbm, wk_hbm, wv_hbm, q_out, kv_out,
           rows, gain, wq, wkv, wflat, oq, okv,
           local_sem, send_sem, recv_sem, z_recv, xy_recv, okv_recv, keep_sem):
    dp, tp = lax.axis_index("dp"), lax.axis_index("tp")
    z, c = tp // CORES, tp % CORES
    grid_x, grid_y = dp // side, dp % side
    odd_x, odd_y = grid_x % 2, grid_y % 2
    quarter = 2 * odd_x + odd_y
    quarter_x, quarter_y, quarter_d = 2 * (1 - odd_x) + odd_y, 2 * odd_x + 1 - odd_y, 3 - quarter
    x_peer = (dp + side * (1 - 2 * odd_x), tp)
    y_peer = (dp + 1 - 2 * odd_y, tp)
    partner = (dp, tp + 1 - 2 * c)

    own, depth = x_hbm.shape
    chip_rows = CORES * own
    step = depth // CHUNKS
    piece = wk_hbm.shape[0]
    tiles = chip_rows // TILE

    def at_ring(distance):
        return (dp, CORES * ((z + ring - distance) % ring) + c)

    def remote(src, dst, send, recv, device):
        return pltpu.make_async_remote_copy(src_ref=src, dst_ref=dst, send_sem=send, recv_sem=recv, device_id=device, device_id_type=MESH)

    def part(block, chunk):
        first = pl.multiple_of(chunk * step, step)
        return wq.at[block, pl.ds(first, step)], wkv.at[block, chunk]

    barrier = pltpu.get_barrier_semaphore()
    above, below = CORES * ((z + 1) % ring), CORES * ((z + ring - 1) % ring)
    peers = [x_peer, y_peer, partner] + [at_ring(1), at_ring(ring - 1)] + [(dp, above + 1 - c), (dp, below + 1 - c)]
    for peer in peers:
        pl.semaphore_signal(barrier, inc=1, device_id=peer, device_id_type=MESH)

    own_first = pl.multiple_of(c * own, own)
    lane = own // 4
    x_loads = [pltpu.make_async_copy(x_hbm.at[pl.ds(i * lane, lane)], rows.at[pl.ds(own_first + i * lane, lane)], local_sem.at[i]) for i in range(4)]
    w_loads = []
    for i in range(QUARTERS):
        first = pl.multiple_of(((quarter + i) % QUARTERS) * (depth // QUARTERS), depth // QUARTERS)
        w_loads.append(pltpu.make_async_copy(wq_hbm.at[pl.ds(first, depth // QUARTERS)], wq.at[z, pl.ds(first, depth // QUARTERS)], local_sem.at[4 + min(i, 1)]))
    gain_load = pltpu.make_async_copy(gain_hbm, gain, local_sem.at[6])
    own_half = pl.ds(pl.multiple_of(c * piece, piece), piece)

    def columns(i):
        chunk = (HALVES * quarter + i) % CHUNKS
        return chunk, pl.ds(pl.multiple_of(chunk * step, step), step)

    def pair_load(source, i):
        chunk, span = columns(i)
        return pltpu.make_async_copy(source.at[:, span], wkv.at[z, chunk, own_half], local_sem.at[7])

    def pair_copy(source, i):
        chunk, span = columns(i)
        return remote(source.at[:, span], wkv.at[z, chunk, own_half], send_sem.at[PAIRS], recv_sem.at[3], partner)

    def pair_wait():
        pieces = wkv.at[z, :, own_half]
        remote(pieces, pieces, send_sem.at[PAIRS], recv_sem.at[3], partner).wait_recv()

    w_loads[0].start()
    for load in x_loads:
        load.start()
    gain_load.start()

    @pl.when(c == 0)
    def _():
        for i in range(CHUNKS):
            pair_load(wk_hbm, i).start()

    @pl.when(c == 1)
    def _():
        for i in range(CHUNKS):
            pair_load(wv_hbm, i).start()

    for load in w_loads[1:]:
        load.start()

    pl.semaphore_wait(barrier, len(peers))

    def pair_start():
        @pl.when(c == 0)
        def _():
            for i in range(CHUNKS):
                pair_copy(wv_hbm, i).start()

        @pl.when(c == 1)
        def _():
            for i in range(CHUNKS):
                pair_copy(wk_hbm, i).start()

    half_ring = ring // 2

    def ring_send(direction, hop, half, kind):
        back = hop if direction == 0 else ring - hop
        block = (z + ring - back) % ring
        reference = part(block, HALVES * quarter + half)[kind]
        copy = remote(reference, reference, send_sem.at[kind], z_recv.at[(hop * HALVES + half) * 2 + kind], at_ring(ring - 1 if direction == 0 else 1))
        copy.start()

    def reach(direction, half):
        return half_ring if direction == half else half_ring - 1

    def key_value_start(half):
        chunk, span = columns(half)
        for direction in range(2):
            landed = 1 if direction == 0 else ring - 1
            for core, source in enumerate((wk_hbm, wv_hbm)):
                device = (dp, CORES * ((z + landed) % ring) + core)
                remote(source.at[:, span], wkv.at[z, chunk, own_half], send_sem.at[1], z_recv.at[half * 2 + 1], device).start()

    def query_start(half):
        span = pl.ds(pl.multiple_of((HALVES * quarter + half) * step, step), step)
        for direction in range(2):
            landed = 1 if direction == 0 else ring - 1
            remote(wq_hbm.at[span], wq.at[z, span], send_sem.at[0], z_recv.at[half * 2], at_ring(ring - landed)).start()

    def ring_service(hop, kind, half):
        directions = [d for d in range(2) if hop <= reach(d, half)]
        arrived = (wq.at[0, pl.ds(0, len(directions) * step)], wkv.at[0, pl.ds(0, len(directions))])[kind]
        remote(arrived, arrived, send_sem.at[kind], z_recv.at[((hop - 1) * HALVES + half) * 2 + kind], partner).wait_recv()
        for direction in directions:
            if hop < reach(direction, half):
                ring_send(direction, hop, half, kind)

    def square_copy(r, lane_index, chunk, kind, device):
        block = (z + ring - r) % ring
        reference = part(block, chunk)[kind]
        index = ((r - 1) * 3 + {0: 0, 3: 1}.get(lane_index, 2)) * 2 + kind
        return remote(reference, reference, send_sem.at[kind], xy_recv.at[index], device)

    def square_send(r, kind, half):
        for base, device in ((0, x_peer), (2, y_peer)):
            square_copy(r, base + half, HALVES * quarter + half, kind, device).start()

    def square_forward(r, kind, half):
        lane_index, chunk, device = ((0, HALVES * quarter_x, y_peer), (3, HALVES * quarter_y + 1, x_peer))[half]
        square_copy(r, lane_index, chunk, kind, device).wait_recv()
        square_copy(r, 4 + half, chunk, kind, device).start()

    def square_rest(r, kind):
        block = (z + ring - r) % ring
        four = (wq.at[block, pl.ds(0, 4 * step)], wkv.at[block, pl.ds(0, 4)])[kind]
        remote(four, four, send_sem.at[kind], xy_recv.at[((r - 1) * 3 + 2) * 2 + kind], x_peer).wait_recv()

    def flatten(block):
        @pl.loop(0, CHUNKS)
        def _(i):
            span = pl.ds(pl.multiple_of(i * step, step), step)
            wflat[span, :] = wq[block, span].reshape(step, wflat.shape[1])

    def product(block, slot, kind, first):
        span = pl.ds(first, TILE)
        if kind == 0:
            q = jnp.dot(rows[span, :], wflat[...], preferred_element_type=jnp.float32)
            oq[slot, span] = q.reshape((TILE,) + oq.shape[2:]).astype(oq.dtype)
        else:
            kv = jnp.zeros((TILE, okv.shape[2]), jnp.float32)
            for i in range(CHUNKS):
                kv += lax.dot_general(rows[span, pl.ds(i * step, step)], wkv[block, i], (((1,), (1,)), ((), ())), preferred_element_type=jnp.float32)
            okv[slot, span] = kv.astype(okv.dtype)

    def out_rows(block, first, count):
        return pl.ds(pl.multiple_of(block * chip_rows + first, TILE), count)

    def out_copy(r, kind, first, count):
        span, target = pl.ds(first, count), out_rows(z, first, count)
        if kind == 0:
            return remote(oq.at[r, span], q_out.at[target], send_sem.at[PRODUCTS], recv_sem.at[0], at_ring(r))
        return remote(okv.at[r, span], kv_out.at[c, target], send_sem.at[PRODUCTS + 1], okv_recv.at[r - 1], at_ring(r))

    def multiply(r, kind):
        block = (z + ring - r) % ring
        if kind == 0:
            flatten(block)

        @pl.loop(0, tiles)
        def _(t):
            first = pl.multiple_of(t * TILE, TILE)
            product(block, r, kind, first)
            if r:
                out_copy(r, kind, first, TILE).start()

    def keep_copy(kind):
        target = out_rows(z, 0, chip_rows)
        source, kept = ((oq.at[0], q_out.at[target]), (okv.at[0], kv_out.at[c, target]))[kind]
        return pltpu.make_async_copy(source, kept, keep_sem.at[kind])

    def hand_over(r, source):
        target = out_rows((z + r) % ring, 0, chip_rows)
        return remote(source, kv_out.at[c, target], send_sem.at[HANDED], recv_sem.at[1], partner)

    def relay(r):
        target = out_rows((z + r) % ring, 0, chip_rows)
        remote(okv.at[r], kv_out.at[c, target], send_sem.at[PRODUCTS + 1], okv_recv.at[r - 1], at_ring(r)).wait_recv()
        hand_over(r, kv_out.at[c, target]).start()

    for half in range(HALVES):
        key_value_start(half)
    for half in range(HALVES):
        query_start(half)
    pair_start()
    for i in range(CHUNKS):
        pair_load(wk_hbm, i).wait()
    gain_load.wait()

    def row_copy(i, core):
        span = pl.ds(pl.multiple_of(core * own + i * lane, lane), lane)
        return remote(rows.at[span], rows.at[span], send_sem.at[ROWS], recv_sem.at[2], partner)

    def half_rows(core):
        span = pl.ds(pl.multiple_of(core * own, own), own)
        return remote(rows.at[span], rows.at[span], send_sem.at[ROWS], recv_sem.at[2], partner)

    def norm(i):
        x_loads[i].wait()

        @pl.loop(0, lane // NORM_ROWS)
        def _(n):
            span = pl.ds(pl.multiple_of(own_first + i * lane + n * NORM_ROWS, NORM_ROWS), NORM_ROWS)
            wide = rows[span, :].astype(jnp.float32)
            mean_sq = jnp.mean(wide * wide, axis=-1, keepdims=True)
            rows[span, :] = (wide * lax.rsqrt(mean_sq + EPSILON) * gain[...]).astype(rows.dtype)

        row_copy(i, c).start()

    normed = 0
    rows_complete = False
    for action, r, kind, half in SCHEDULE:
        if action in (MULTIPLY, OWN) and not rows_complete:
            rows_complete = True
            half_rows(1 - c).wait_recv()
        if action == ARRIVE:
            ring_service(r, kind, half)
        elif action == SPREAD:
            square_send(r, kind, half)
        elif action == FORWARD:
            square_forward(r, kind, half)
        elif action == MULTIPLY:
            square_rest(r, kind)
            multiply(r, kind)
        elif action == HAND_OVER:
            relay(r)
        elif action == NORM:
            norm(normed)
            normed += 1
        elif kind == 0:
            for load in w_loads:
                load.wait()
            multiply(0, 0)
            keep_copy(0).start()
        else:
            pair_wait()
            multiply(0, 1)
            keep_copy(1).start()
            hand_over(0, okv.at[0]).start()

    for kind in range(2):
        keep_copy(kind).wait()

    def whole(source, target, send, recv):
        return remote(source, target, send_sem.at[send], recv_sem.at[recv], partner)

    others = ring - 1
    products = q_out.at[pl.ds(0, others * chip_rows)]
    whole(products, products, PRODUCTS, 0).wait_recv()
    heads = kv_out.at[1 - c]
    whole(heads, heads, HANDED, 1).wait()
    half_rows(c).wait_send()
    for kind, weights in enumerate((wq, wkv)):
        sent = weights.at[pl.ds(0, others)]
        whole(sent, sent, kind, 0).wait_send()
    for kind, buffer in enumerate((oq, okv)):
        sent = buffer.at[pl.ds(0, others)]
        whole(sent, sent, PRODUCTS + kind, 0).wait_send()
    pieces = wkv.at[z, :, own_half]
    whole(pieces, pieces, PAIRS, 0).wait_send()


def flush(q_ref, kv_ref, q_out, k_out, v_out, sem):
    copies = [pltpu.make_async_copy(source, target, sem.at[i]) for i, (source, target) in enumerate(((q_ref, q_out), (kv_ref.at[0], k_out), (kv_ref.at[1], v_out)))]
    for copy in copies:
        copy.start()
    for copy in copies:
        copy.wait()


def solution(mesh):
    ring = mesh.shape["tp"] // CORES
    side = math.isqrt(mesh.shape["dp"])
    assert side * side == mesh.shape["dp"] and side % 2 == 0

    def local_step(x_rows, norm_gain, w_q, w_k, w_v):
        own, depth = x_rows.shape
        heads, width = w_q.shape[1:]
        piece = w_k.shape[1]
        assert piece * CORES == width
        tokens, chip_rows, step = own * CORES * ring, own * CORES, depth // CHUNKS
        dma = pltpu.SemaphoreType.DMA
        bf16 = x_rows.dtype
        q_out, kv_out = pl.pallas_call(
            functools.partial(kernel, ring, side),
            out_shape=(
                jax.ShapeDtypeStruct((tokens, heads, width), bf16),
                jax.ShapeDtypeStruct((CORES, tokens, width), bf16),
            ),
            in_specs=[pl.BlockSpec(memory_space=pltpu.HBM)] * 5,
            out_specs=(pl.BlockSpec(memory_space=pl.ANY),) * 2,
            scratch_shapes=[
                pltpu.VMEM((chip_rows, depth), bf16),
                pltpu.VMEM((1, depth), jnp.float32),
                pltpu.VMEM((ring, depth, heads, width), bf16),
                pltpu.VMEM((ring, CHUNKS, width, step), bf16),
                pltpu.VMEM((depth, heads * width), bf16),
                pltpu.VMEM((ring, chip_rows, heads, width), bf16),
                pltpu.VMEM((ring, chip_rows, width), bf16),
                dma((8,)), dma((HANDED + 1,)), dma((4,)),
                dma((ring // 2 * HALVES * 2,)), dma(((ring - 1) * 3 * 2,)), dma((ring - 1,)), dma((2,)),
            ],
            compiler_params=pltpu.CompilerParams(collective_id=0, has_side_effects=True, vmem_limit_bytes=42 * 1024 * 1024),
        )(*(pltpu.with_memory_space_constraint(a, pltpu.HBM) for a in (x_rows, norm_gain.reshape(1, depth), w_q, w_k.T, w_v.T)))
        head = jax.ShapeDtypeStruct((tokens, width), bf16)
        q_out, k_out, v_out = pl.pallas_call(
            flush,
            out_shape=(jax.ShapeDtypeStruct((tokens, heads, width), bf16), head, head),
            in_specs=[pl.BlockSpec(memory_space=pl.ANY)] * 2,
            out_specs=(pl.BlockSpec(memory_space=pl.ANY),) * 3,
            scratch_shapes=[dma((3,))],
            compiler_params=pltpu.CompilerParams(vmem_limit_bytes=1024 * 1024),
        )(q_out, kv_out)
        return q_out, k_out[:, None, :], v_out[:, None, :]

    return jax.shard_map(local_step, mesh=mesh, in_specs=(P(("dp", "tp"), None), P(None), P(None, "tp", None), P(None, "tp"), P(None, "tp")), out_specs=(P("dp", "tp", None), P("dp", "tp", None), P("dp", "tp", None)), check_vma=False)
```

```python
import functools
import math

import jax
import jax.numpy as jnp
from jax import lax
from jax.experimental import pallas as pl
from jax.experimental.pallas import tpu as pltpu
from jax.sharding import PartitionSpec as P

EPSILON = 1e-6
MESH = pl.DeviceIdType.MESH
CORES = 2
QUARTERS = 4
HALVES = 2
CHUNKS = QUARTERS * HALVES
TILE = 128
NORM_ROWS = 16

PAIRS, PRODUCTS, ROWS, HANDED = 2, 3, 5, 6

ARRIVE, SPREAD, FORWARD, MULTIPLY, HAND_OVER, NORM, OWN = range(7)
SCHEDULE = (
    (NORM, 0, 0, 0), (ARRIVE, 1, 1, 0), (SPREAD, 7, 1, 0), (ARRIVE, 1, 1, 1), (SPREAD, 1, 1, 0),
    (SPREAD, 7, 1, 1), (SPREAD, 1, 1, 1), (FORWARD, 1, 1, 0), (FORWARD, 7, 1, 0), (FORWARD, 7, 1, 1),
    (ARRIVE, 1, 0, 1), (FORWARD, 1, 1, 1), (ARRIVE, 2, 1, 0), (SPREAD, 2, 1, 0), (NORM, 0, 0, 0),
    (ARRIVE, 2, 1, 1), (SPREAD, 6, 1, 0), (NORM, 0, 0, 0), (SPREAD, 6, 1, 1), (ARRIVE, 1, 0, 0),
    (NORM, 0, 0, 0), (SPREAD, 2, 1, 1), (ARRIVE, 2, 0, 1), (SPREAD, 6, 0, 1), (FORWARD, 2, 1, 1),
    (ARRIVE, 3, 1, 0), (ARRIVE, 3, 1, 1), (SPREAD, 5, 1, 1), (ARRIVE, 2, 0, 0), (FORWARD, 2, 1, 0),
    (SPREAD, 5, 1, 0), (ARRIVE, 3, 0, 1), (SPREAD, 3, 0, 1), (MULTIPLY, 7, 1, 0), (FORWARD, 5, 1, 0),
    (FORWARD, 5, 1, 1), (MULTIPLY, 2, 1, 0), (ARRIVE, 3, 0, 0), (SPREAD, 3, 0, 0), (SPREAD, 6, 0, 0),
    (MULTIPLY, 1, 1, 0), (ARRIVE, 4, 1, 1), (FORWARD, 3, 0, 1), (MULTIPLY, 5, 1, 0), (ARRIVE, 4, 1, 0),
    (FORWARD, 6, 0, 1), (OWN, 0, 1, 0), (FORWARD, 3, 0, 0), (FORWARD, 6, 0, 0), (SPREAD, 4, 1, 1),
    (ARRIVE, 4, 0, 1), (ARRIVE, 4, 0, 0), (SPREAD, 5, 0, 1), (SPREAD, 4, 1, 0), (SPREAD, 3, 1, 1),
    (FORWARD, 6, 1, 0), (MULTIPLY, 3, 0, 0), (SPREAD, 4, 0, 1), (MULTIPLY, 6, 0, 0), (FORWARD, 6, 1, 1),
    (FORWARD, 4, 1, 0), (OWN, 0, 0, 0), (SPREAD, 3, 1, 0), (FORWARD, 4, 1, 1), (SPREAD, 5, 0, 0),
    (MULTIPLY, 6, 1, 0), (SPREAD, 4, 0, 0), (FORWARD, 3, 1, 1), (FORWARD, 3, 1, 0), (MULTIPLY, 4, 1, 0),
    (FORWARD, 5, 0, 1), (FORWARD, 5, 0, 0), (SPREAD, 7, 0, 0), (MULTIPLY, 3, 1, 0), (HAND_OVER, 7, 1, 0),
    (FORWARD, 4, 0, 0), (FORWARD, 4, 0, 1), (HAND_OVER, 1, 1, 0), (MULTIPLY, 5, 0, 0), (SPREAD, 2, 0, 1),
    (SPREAD, 2, 0, 0), (MULTIPLY, 4, 0, 0), (SPREAD, 1, 0, 1), (FORWARD, 2, 0, 0), (FORWARD, 2, 0, 1),
    (SPREAD, 1, 0, 0), (SPREAD, 7, 0, 1), (MULTIPLY, 2, 0, 0), (FORWARD, 1, 0, 1), (FORWARD, 1, 0, 0),
    (HAND_OVER, 6, 1, 0), (HAND_OVER, 4, 1, 0), (FORWARD, 7, 0, 1), (FORWARD, 7, 0, 0), (MULTIPLY, 1, 0, 0),
    (MULTIPLY, 7, 0, 0), (HAND_OVER, 5, 1, 0), (HAND_OVER, 3, 1, 0), (HAND_OVER, 2, 1, 0),
)


def kernel(ring, side, x_hbm, gain_hbm, wq_hbm, wk_hbm, wv_hbm, q_out, kv_out,
           rows, gain, wq, wkv, wflat, oq, okv,
           local_sem, send_sem, recv_sem, z_recv, xy_recv, okv_recv, keep_sem):
    dp, tp = lax.axis_index("dp"), lax.axis_index("tp")
    z, c = tp // CORES, tp % CORES
    grid_x, grid_y = dp // side, dp % side
    odd_x, odd_y = grid_x % 2, grid_y % 2
    quarter = 2 * odd_x + odd_y
    quarter_x, quarter_y, quarter_d = 2 * (1 - odd_x) + odd_y, 2 * odd_x + 1 - odd_y, 3 - quarter
    x_peer = (dp + side * (1 - 2 * odd_x), tp)
    y_peer = (dp + 1 - 2 * odd_y, tp)
    partner = (dp, tp + 1 - 2 * c)

    own, depth = x_hbm.shape
    chip_rows = CORES * own
    step = depth // CHUNKS
    piece = wk_hbm.shape[0]
    tiles = chip_rows // TILE

    def at_ring(distance):
        return (dp, CORES * ((z + ring - distance) % ring) + c)

    def remote(src, dst, send, recv, device):
        return pltpu.make_async_remote_copy(src_ref=src, dst_ref=dst, send_sem=send, recv_sem=recv, device_id=device, device_id_type=MESH)

    def part(block, chunk):
        first = pl.multiple_of(chunk * step, step)
        return wq.at[block, pl.ds(first, step)], wkv.at[block, chunk]

    barrier = pltpu.get_barrier_semaphore()
    above, below = CORES * ((z + 1) % ring), CORES * ((z + ring - 1) % ring)
    peers = [x_peer, y_peer, partner] + [at_ring(1), at_ring(ring - 1)] + [(dp, above + 1 - c), (dp, below + 1 - c)]
    for peer in peers:
        pl.semaphore_signal(barrier, inc=1, device_id=peer, device_id_type=MESH)

    own_first = pl.multiple_of(c * own, own)
    lane = own // 4
    x_loads = [pltpu.make_async_copy(x_hbm.at[pl.ds(i * lane, lane)], rows.at[pl.ds(own_first + i * lane, lane)], local_sem.at[i]) for i in range(4)]
    w_loads = []
    for i in range(QUARTERS):
        first = pl.multiple_of(((quarter + i) % QUARTERS) * (depth // QUARTERS), depth // QUARTERS)
        w_loads.append(pltpu.make_async_copy(wq_hbm.at[pl.ds(first, depth // QUARTERS)], wq.at[z, pl.ds(first, depth // QUARTERS)], local_sem.at[4 + min(i, 1)]))
    gain_load = pltpu.make_async_copy(gain_hbm, gain, local_sem.at[6])
    own_half = pl.ds(pl.multiple_of(c * piece, piece), piece)

    def columns(i):
        chunk = (HALVES * quarter + i) % CHUNKS
        return chunk, pl.ds(pl.multiple_of(chunk * step, step), step)

    def pair_load(source, i):
        chunk, span = columns(i)
        return pltpu.make_async_copy(source.at[:, span], wkv.at[z, chunk, own_half], local_sem.at[7])

    def pair_copy(source, i):
        chunk, span = columns(i)
        return remote(source.at[:, span], wkv.at[z, chunk, own_half], send_sem.at[PAIRS], recv_sem.at[3], partner)

    def pair_wait():
        pieces = wkv.at[z, :, own_half]
        remote(pieces, pieces, send_sem.at[PAIRS], recv_sem.at[3], partner).wait_recv()

    for load in x_loads:
        load.start()
    gain_load.start()

    pl.semaphore_wait(barrier, len(peers))

    def pair_start():
        @pl.when(c == 0)
        def _():
            for i in range(CHUNKS):
                pair_copy(wv_hbm, i).start()

        @pl.when(c == 1)
        def _():
            for i in range(CHUNKS):
                pair_copy(wk_hbm, i).start()

    half_ring = ring // 2

    def ring_send(direction, hop, half, kind):
        back = hop if direction == 0 else ring - hop
        block = (z + ring - back) % ring
        reference = part(block, HALVES * quarter + half)[kind]
        copy = remote(reference, reference, send_sem.at[kind], z_recv.at[(hop * HALVES + half) * 2 + kind], at_ring(ring - 1 if direction == 0 else 1))
        copy.start()

    def reach(direction, half):
        return half_ring if direction == half else half_ring - 1

    def key_value_start(half):
        chunk, span = columns(half)
        for direction in range(2):
            landed = 1 if direction == 0 else ring - 1
            for core, source in enumerate((wk_hbm, wv_hbm)):
                device = (dp, CORES * ((z + landed) % ring) + core)
                remote(source.at[:, span], wkv.at[z, chunk, own_half], send_sem.at[1], z_recv.at[half * 2 + 1], device).start()

    def query_start(half):
        span = pl.ds(pl.multiple_of((HALVES * quarter + half) * step, step), step)
        for direction in range(2):
            landed = 1 if direction == 0 else ring - 1
            remote(wq_hbm.at[span], wq.at[z, span], send_sem.at[0], z_recv.at[half * 2], at_ring(ring - landed)).start()

    def ring_service(hop, kind, half):
        directions = [d for d in range(2) if hop <= reach(d, half)]
        arrived = (wq.at[0, pl.ds(0, len(directions) * step)], wkv.at[0, pl.ds(0, len(directions))])[kind]
        remote(arrived, arrived, send_sem.at[kind], z_recv.at[((hop - 1) * HALVES + half) * 2 + kind], partner).wait_recv()
        for direction in directions:
            if hop < reach(direction, half):
                ring_send(direction, hop, half, kind)

    def square_copy(r, lane_index, chunk, kind, device):
        block = (z + ring - r) % ring
        reference = part(block, chunk)[kind]
        index = ((r - 1) * 3 + {0: 0, 3: 1}.get(lane_index, 2)) * 2 + kind
        return remote(reference, reference, send_sem.at[kind], xy_recv.at[index], device)

    def square_send(r, kind, half):
        for base, device in ((0, x_peer), (2, y_peer)):
            square_copy(r, base + half, HALVES * quarter + half, kind, device).start()

    def square_forward(r, kind, half):
        lane_index, chunk, device = ((0, HALVES * quarter_x, y_peer), (3, HALVES * quarter_y + 1, x_peer))[half]
        square_copy(r, lane_index, chunk, kind, device).wait_recv()
        square_copy(r, 4 + half, chunk, kind, device).start()

    def square_rest(r, kind):
        block = (z + ring - r) % ring
        four = (wq.at[block, pl.ds(0, 4 * step)], wkv.at[block, pl.ds(0, 4)])[kind]
        remote(four, four, send_sem.at[kind], xy_recv.at[((r - 1) * 3 + 2) * 2 + kind], x_peer).wait_recv()

    def flatten(block):
        @pl.loop(0, CHUNKS)
        def _(i):
            span = pl.ds(pl.multiple_of(i * step, step), step)
            wflat[span, :] = wq[block, span].reshape(step, wflat.shape[1])

    def product(block, slot, kind, first):
        span = pl.ds(first, TILE)
        if kind == 0:
            q = jnp.dot(rows[span, :], wflat[...], preferred_element_type=jnp.float32)
            oq[slot, span] = q.reshape((TILE,) + oq.shape[2:]).astype(oq.dtype)
        else:
            kv = jnp.zeros((TILE, okv.shape[2]), jnp.float32)
            for i in range(CHUNKS):
                kv += lax.dot_general(rows[span, pl.ds(i * step, step)], wkv[block, i], (((1,), (1,)), ((), ())), preferred_element_type=jnp.float32)
            okv[slot, span] = kv.astype(okv.dtype)

    def out_rows(block, first, count):
        return pl.ds(pl.multiple_of(block * chip_rows + first, TILE), count)

    def out_copy(r, kind, first, count):
        span, target = pl.ds(first, count), out_rows(z, first, count)
        if kind == 0:
            return remote(oq.at[r, span], q_out.at[target], send_sem.at[PRODUCTS], recv_sem.at[0], at_ring(r))
        return remote(okv.at[r, span], kv_out.at[c, target], send_sem.at[PRODUCTS + 1], okv_recv.at[r - 1], at_ring(r))

    def multiply(r, kind):
        block = (z + ring - r) % ring
        if kind == 0:
            flatten(block)

        @pl.loop(0, tiles)
        def _(t):
            first = pl.multiple_of(t * TILE, TILE)
            product(block, r, kind, first)
            if r:
                out_copy(r, kind, first, TILE).start()

    def keep_copy(kind):
        target = out_rows(z, 0, chip_rows)
        source, kept = ((oq.at[0], q_out.at[target]), (okv.at[0], kv_out.at[c, target]))[kind]
        return pltpu.make_async_copy(source, kept, keep_sem.at[kind])

    def hand_over(r, source):
        target = out_rows((z + r) % ring, 0, chip_rows)
        return remote(source, kv_out.at[c, target], send_sem.at[HANDED], recv_sem.at[1], partner)

    def relay(r):
        target = out_rows((z + r) % ring, 0, chip_rows)
        remote(okv.at[r], kv_out.at[c, target], send_sem.at[PRODUCTS + 1], okv_recv.at[r - 1], at_ring(r)).wait_recv()
        hand_over(r, kv_out.at[c, target]).start()

    for half in range(HALVES):
        key_value_start(half)
    for half in range(HALVES):
        query_start(half)
    @pl.when(c == 0)
    def _():
        for i in range(CHUNKS):
            pair_load(wk_hbm, i).start()

    @pl.when(c == 1)
    def _():
        for i in range(CHUNKS):
            pair_load(wv_hbm, i).start()

    for load in w_loads:
        load.start()

    pair_start()
    for i in range(CHUNKS):
        pair_load(wk_hbm, i).wait()
    gain_load.wait()

    def row_copy(i, core):
        span = pl.ds(pl.multiple_of(core * own + i * lane, lane), lane)
        return remote(rows.at[span], rows.at[span], send_sem.at[ROWS], recv_sem.at[2], partner)

    def half_rows(core):
        span = pl.ds(pl.multiple_of(core * own, own), own)
        return remote(rows.at[span], rows.at[span], send_sem.at[ROWS], recv_sem.at[2], partner)

    def norm(i):
        x_loads[i].wait()

        @pl.loop(0, lane // NORM_ROWS)
        def _(n):
            span = pl.ds(pl.multiple_of(own_first + i * lane + n * NORM_ROWS, NORM_ROWS), NORM_ROWS)
            wide = rows[span, :].astype(jnp.float32)
            mean_sq = jnp.mean(wide * wide, axis=-1, keepdims=True)
            rows[span, :] = (wide * lax.rsqrt(mean_sq + EPSILON) * gain[...]).astype(rows.dtype)

        row_copy(i, c).start()

    normed = 0
    rows_complete = False
    for action, r, kind, half in SCHEDULE:
        if action in (MULTIPLY, OWN) and not rows_complete:
            rows_complete = True
            half_rows(1 - c).wait_recv()
        if action == ARRIVE:
            ring_service(r, kind, half)
        elif action == SPREAD:
            square_send(r, kind, half)
        elif action == FORWARD:
            square_forward(r, kind, half)
        elif action == MULTIPLY:
            square_rest(r, kind)
            multiply(r, kind)
        elif action == HAND_OVER:
            relay(r)
        elif action == NORM:
            norm(normed)
            normed += 1
        elif kind == 0:
            for load in w_loads:
                load.wait()
            multiply(0, 0)
            keep_copy(0).start()
        else:
            pair_wait()
            multiply(0, 1)
            keep_copy(1).start()
            hand_over(0, okv.at[0]).start()

    for kind in range(2):
        keep_copy(kind).wait()

    def whole(source, target, send, recv):
        return remote(source, target, send_sem.at[send], recv_sem.at[recv], partner)

    others = ring - 1
    products = q_out.at[pl.ds(0, others * chip_rows)]
    whole(products, products, PRODUCTS, 0).wait_recv()
    heads = kv_out.at[1 - c]
    whole(heads, heads, HANDED, 1).wait()
    half_rows(c).wait_send()
    for kind, weights in enumerate((wq, wkv)):
        sent = weights.at[pl.ds(0, others)]
        whole(sent, sent, kind, 0).wait_send()
    for kind, buffer in enumerate((oq, okv)):
        sent = buffer.at[pl.ds(0, others)]
        whole(sent, sent, PRODUCTS + kind, 0).wait_send()
    pieces = wkv.at[z, :, own_half]
    whole(pieces, pieces, PAIRS, 0).wait_send()


def flush(q_ref, kv_ref, q_out, k_out, v_out, sem):
    copies = [pltpu.make_async_copy(source, target, sem.at[i]) for i, (source, target) in enumerate(((q_ref, q_out), (kv_ref.at[0], k_out), (kv_ref.at[1], v_out)))]
    for copy in copies:
        copy.start()
    for copy in copies:
        copy.wait()


def solution(mesh):
    ring = mesh.shape["tp"] // CORES
    side = math.isqrt(mesh.shape["dp"])
    assert side * side == mesh.shape["dp"] and side % 2 == 0

    def local_step(x_rows, norm_gain, w_q, w_k, w_v):
        own, depth = x_rows.shape
        heads, width = w_q.shape[1:]
        piece = w_k.shape[1]
        assert piece * CORES == width
        tokens, chip_rows, step = own * CORES * ring, own * CORES, depth // CHUNKS
        dma = pltpu.SemaphoreType.DMA
        bf16 = x_rows.dtype
        q_out, kv_out = pl.pallas_call(
            functools.partial(kernel, ring, side),
            out_shape=(
                jax.ShapeDtypeStruct((tokens, heads, width), bf16),
                jax.ShapeDtypeStruct((CORES, tokens, width), bf16),
            ),
            in_specs=[pl.BlockSpec(memory_space=pltpu.HBM)] * 5,
            out_specs=(pl.BlockSpec(memory_space=pl.ANY),) * 2,
            scratch_shapes=[
                pltpu.VMEM((chip_rows, depth), bf16),
                pltpu.VMEM((1, depth), jnp.float32),
                pltpu.VMEM((ring, depth, heads, width), bf16),
                pltpu.VMEM((ring, CHUNKS, width, step), bf16),
                pltpu.VMEM((depth, heads * width), bf16),
                pltpu.VMEM((ring, chip_rows, heads, width), bf16),
                pltpu.VMEM((ring, chip_rows, width), bf16),
                dma((8,)), dma((HANDED + 1,)), dma((4,)),
                dma((ring // 2 * HALVES * 2,)), dma(((ring - 1) * 3 * 2,)), dma((ring - 1,)), dma((2,)),
            ],
            compiler_params=pltpu.CompilerParams(collective_id=0, has_side_effects=True, vmem_limit_bytes=42 * 1024 * 1024),
        )(*(pltpu.with_memory_space_constraint(a, pltpu.HBM) for a in (x_rows, norm_gain.reshape(1, depth), w_q, w_k.T, w_v.T)))
        head = jax.ShapeDtypeStruct((tokens, width), bf16)
        q_out, k_out, v_out = pl.pallas_call(
            flush,
            out_shape=(jax.ShapeDtypeStruct((tokens, heads, width), bf16), head, head),
            in_specs=[pl.BlockSpec(memory_space=pl.ANY)] * 2,
            out_specs=(pl.BlockSpec(memory_space=pl.ANY),) * 3,
            scratch_shapes=[dma((3,))],
            compiler_params=pltpu.CompilerParams(vmem_limit_bytes=1024 * 1024),
        )(q_out, kv_out)
        return q_out, k_out[:, None, :], v_out[:, None, :]

    return jax.shard_map(local_step, mesh=mesh, in_specs=(P(("dp", "tp"), None), P(None), P(None, "tp", None), P(None, "tp"), P(None, "tp")), out_specs=(P("dp", "tp", None), P("dp", "tp", None), P("dp", "tp", None)), check_vma=False)
```
